32 devices in a mesh: member: 4 (over y, core), space: 8 (over z, x).
Axes of the slice: x: 2, y: 2, z: 4, core: 2. Of those that a mesh axis runs over, the one named last changes fastest.
Arguments:
- participant_swirls: float32 [8, 512, 512], P('member', 'space'), may hold values from -6 to 6
- driving_source: float32 [512, 512], P('space'), may hold values from -12 to 12
- mixing: float32 [8, 8], replicated, may hold values from -2 to 2
- probes: int32 [16384], P('space'), may hold values from 0 to 32767
- observed: float32 [16384], P('space'), may hold values from -6 to 6
Outputs:
- analysis: float32 [8, 512, 512], P('member', 'space')
- spread: float32 [8, 8], replicated
- projection: float32 [8], replicated
The draws below stay inside these ranges and needn't reach their ends.
Inputs may be any that keep to these rules, and one draw needn't show every extreme that they name: `probes`: each index names a cell of its own block's 64 rows, row-major with 512 columns.
All inputs are finite; a program needn't handle non-finite values.
Results may differ from the reference program's by a relative error of at most 0.0003.
Values may be sent and summed in bfloat16 or wider, within the bound.
No kernel may reach another device: no remote copies, remote signals or barrier semaphores. Data moves between devices by JAX's collectives and lax.ppermute only.
A program may use at most 64 MiB of HBM per device.

```python
import math
import jax
import jax.numpy as jnp
from jax import lax

N = 512
KEEP = 160
PROBE_DEV = 2048
MEMBERS = 8
ROWS = 64
PROBES = 16384


def touch_ends(entries, key, low, top_value):
    index_at = [jax.random.randint(jax.random.fold_in(key, axis), (), 0, length) for axis, length in enumerate(entries.shape)]
    main_axis = entries.shape.index(max(entries.shape))
    beside = index_at[:main_axis] + [(index_at[main_axis] + 1) % entries.shape[main_axis]] + index_at[main_axis + 1:]
    return entries.at[tuple(index_at)].set(low).at[tuple(beside)].set(top_value)


def levels(key, shape, split, low, high):
    gain, own = 1.0, jax.random.fold_in(key, 6)
    for axis_at, parts in split:
        steps = jnp.exp(jax.random.uniform(jax.random.fold_in(own, axis_at), (parts,), jnp.float32, low / len(split), high / len(split)))
        gain = gain * jnp.repeat(steps, shape[axis_at] // parts).reshape([-1 if axis == axis_at else 1 for axis in range(len(shape))])
    return gain


def centred(stream_key, shape, scale, bound, cuts=(), kind=jnp.bfloat16):
    level = levels(stream_key, shape, cuts, -0.22, 0.18) if cuts else 1.0
    drawn = jax.random.normal(stream_key, shape, jnp.float32) * scale * level
    return jnp.minimum(jnp.maximum(drawn, -bound), bound).astype(kind)


def setup_inputs(seed: int = 0) -> dict:
    splits = jax.random.split(jax.random.key(seed), 6)
    return {
        "participant_swirls": centred(splits[0], (MEMBERS, N, N), 1.0, 6.0, ((0, 4), (1, 8)), jnp.float32),
        "driving_source": centred(splits[1], (N, N), 2.0, 12.0, ((0, 8),), jnp.float32),
        "mixing": centred(splits[2], (MEMBERS, MEMBERS), MEMBERS ** -0.5, 2.0, (), jnp.float32),
        "probes": touch_ends(jax.random.randint(splits[3], (PROBES,), 0, ROWS * N), jax.random.fold_in(splits[3], 1), 0, (ROWS * N) - 1).astype(jnp.int32),
        "observed": centred(splits[4], (PROBES,), 1.0, 6.0, ((0, 8),), jnp.float32),
    }


DT_STEP = 0.1
VISCOSITY = 0.05

def wave_numbers():
    slots = jnp.arange(2 * KEEP, dtype=jnp.int32)
    along_x = jnp.where(slots < KEEP, slots, slots - 2 * KEEP)
    along_y = jnp.arange(KEEP, dtype=jnp.int32)
    scale = 2.0 * math.pi / N
    wave_x = (along_x.astype(jnp.float32) * scale)[:, None]
    wave_y = (along_y.astype(jnp.float32) * scale)[None, :]
    return (wave_x, wave_y)

def to_modes(field):
    spectrum = jnp.fft.rfft2(field) / (N * N)
    picked = jnp.concatenate([spectrum[:KEEP], spectrum[N - KEEP:]], 0)
    return picked[:, :KEEP]

def to_cells(modes):
    blank = jnp.zeros((N - 2 * KEEP, KEEP), modes.dtype)
    full = jnp.concatenate([modes[:KEEP], blank, modes[KEEP:]], 0)
    full = jnp.pad(full, ((0, 0), (0, N // 2 + 1 - KEEP)))
    return jnp.fft.irfft2(full, s=(N, N)) * (N * N)

def advance_model_once(curl_distribution, driving_source):
    wave_x, wave_y = wave_numbers()
    squared = wave_x * wave_x + wave_y * wave_y
    inverse_sq = jnp.where(squared > 0, 1.0 / jnp.where(squared > 0, squared, 1.0), 0.0)
    spectral = to_modes(curl_distribution)
    stream = spectral * inverse_sq
    vel_x = to_cells(1j * wave_y * stream)
    vel_y = to_cells(-1j * wave_x * stream)
    grad_x = to_cells(1j * wave_x * spectral)
    grad_y = to_cells(1j * wave_y * spectral)
    advect = vel_x * grad_x + vel_y * grad_y
    updated = spectral + DT_STEP * (-to_modes(advect) - VISCOSITY * squared * spectral)
    return to_cells(updated) + DT_STEP * driving_source

def reference(participant_swirls, driving_source, mixing, probes, observed):
    random_perturbations = lax.map(lambda lone_participant: advance_model_once(lone_participant, driving_source), participant_swirls)
    rounded = random_perturbations.astype(jnp.bfloat16)
    values = rounded.astype(jnp.float32)
    mean = lax.optimization_barrier(jnp.mean(values, 0))
    weights = lax.optimization_barrier(jnp.sum(mixing, 0))
    analysis = jnp.einsum('jm,jxy->mxy', mixing, values, precision=lax.Precision.HIGHEST)
    analysis = analysis + (1.0 - weights)[:, None, None] * mean[None]
    block = jnp.arange(PROBES, dtype=jnp.int32) // PROBE_DEV
    cells = block * (ROWS * N) + probes
    picked = values.reshape(MEMBERS, N * N)[:, cells]
    centre = lax.optimization_barrier(jnp.mean(picked, 0))
    anomaly = picked - centre[None]
    spread = jnp.dot(anomaly, anomaly.T, precision=lax.Precision.HIGHEST) / PROBES
    projection = jnp.dot(anomaly, observed - centre, precision=lax.Precision.HIGHEST) / math.sqrt(PROBES)
    return (analysis, spread, projection)
```

```python
import functools
import math

import jax
import jax.numpy as jnp
import numpy as np
from jax import lax
from jax.experimental import pallas as pl
from jax.experimental.pallas import tpu as pltpu
from jax.sharding import PartitionSpec as P

KEEP = 160
DT_STEP = 0.1
VISCOSITY = 0.05
LANES = 128
F32 = jnp.float32
BF16 = jnp.bfloat16

NN = (((1,), (0,)), ((), ()))
NT = (((1,), (1,)), ((), ()))


def round_up(value, unit):
    return -(-value // unit) * unit


def split_table(table):
    high = np.asarray(table, np.float32).astype(BF16)
    low = (np.asarray(table, np.float64) - high.astype(np.float64)).astype(np.float32).astype(BF16)
    return jnp.asarray(high), jnp.asarray(low)


def split_value(value):
    high = value.astype(BF16)
    return high, (value - high.astype(F32)).astype(BF16)


def dot3(left, right, dims):
    def one(a, b):
        return lax.dot_general(a, b, dims, preferred_element_type=F32)

    return one(left[0], right[0]) + (one(left[0], right[1]) + one(left[1], right[0]))


class Plan:
    def __init__(self, n, rows, space, count):
        self.n, self.rows, self.space, self.count = n, rows, space, count
        self.group = space // count
        self.block = round_up(-(-KEEP // self.group), 8)
        self.modes = self.block * self.group
        self.half = n // 2
        self.kpad = round_up(KEEP + 1, LANES)
        cells = np.arange(n) + 0.5
        scale = 2.0 * math.pi / n
        ky = np.arange(self.modes)
        live = (ky < KEEP)[:, None]
        angle_y = scale * ky[:, None] * cells[None, :]
        cos_y, sin_y = np.cos(angle_y) * live, np.sin(angle_y) * live
        self.y_forward = split_table(np.concatenate([cos_y, -sin_y], 0))
        twice = np.where(ky == 0, 1.0, 2.0)[:, None]
        inverse_y = np.stack([(cos_y * twice)[:, : self.half].T, (sin_y * twice)[:, : self.half].T])
        self.y_inverse = split_table(inverse_y)
        own = np.stack([2.0 * cos_y[:, : self.half], 2.0 * sin_y[:, : self.half]])
        own = own.reshape(2, self.group, self.block, self.half).transpose(1, 0, 2, 3)
        self.y_own = split_table(own)
        kx = np.arange(self.kpad)
        angle_x = scale * cells[:, None] * kx[None, :]
        keep_x = (kx <= KEEP)[None, :]
        self.x_table = split_table(np.concatenate([np.cos(angle_x) * keep_x, np.sin(angle_x) * keep_x], 1))


def rows_kernel(plan, field_ref, high_ref, low_ref, out_ref):
    rows, modes = plan.rows, plan.modes
    field = split_value(field_ref[...])
    partial = dot3((high_ref[...], low_ref[...]), field, NT)
    real, imag = partial[:modes], partial[modes:]
    for member in range(plan.count):
        at = slice(member * rows, (member + 1) * rows)
        packed = jnp.concatenate([real[:, at], imag[:, at]], 1)
        for peer in range(plan.group):
            out_ref[member * plan.group + peer] = packed


def project(plan, k_lane, cos_re, cos_im, sin_re, sin_im):
    weight = jnp.where((k_lane == 0) | (k_lane == KEEP), 1.0, 2.0)
    edge = jnp.where(k_lane == KEEP, 1.0, 0.0)
    return (
        weight * cos_re - edge * sin_im,
        weight * cos_im + edge * sin_re,
        weight * sin_re + edge * cos_im,
        weight * sin_im - edge * cos_re,
    )


def member_kernel(plan, own_ref, moved_ref, xh_ref, xl_ref, yih_ref, yil_ref, yoh_ref, yol_ref, out_ref, coef_ref):
    n, half, modes, block, kpad, rows = plan.n, plan.half, plan.modes, plan.block, plan.kpad, plan.rows
    unit = 2.0 * math.pi / n
    own = own_ref[0]

    def x_cos(at=slice(None)):
        return xh_ref[at, :kpad], xl_ref[at, :kpad]

    def x_sin(at=slice(None)):
        return xh_ref[at, kpad:], xl_ref[at, kpad:]

    real = jnp.concatenate([moved_ref[s, :, :rows] for s in range(plan.space)], 1)
    imag = jnp.concatenate([moved_ref[s, :, rows:] for s in range(plan.space)], 1)
    field = split_value(jnp.concatenate([real, imag], 0))
    spectrum = dot3(field, (xh_ref[...], xl_ref[...]), NN)
    sums = (spectrum[:modes, :kpad], spectrum[modes:, :kpad], spectrum[:modes, kpad:], spectrum[modes:, kpad:])
    for part in range(4):
        coef_ref[part] = sums[part]

    def waves(count, first):
        k_lane = lax.broadcasted_iota(jnp.int32, (count, kpad), 1)
        ky_row = lax.broadcasted_iota(jnp.int32, (count, kpad), 0) + first
        wave_x = k_lane.astype(F32) * unit
        wave_y = ky_row.astype(F32) * unit
        return k_lane, wave_x, wave_y, wave_x * wave_x + wave_y * wave_y

    k_lane, wave_x, wave_y, squared = waves(modes, 0)
    live = squared > 0
    inverse_sq = jnp.where(live, 1.0 / jnp.where(live, squared, 1.0), 0.0)
    a_re, a_im, b_re, b_im = project(plan, k_lane, *[s * (1.0 / (n * n)) for s in sums])
    pa_re, pa_im, pb_re, pb_im = (c * inverse_sq for c in (a_re, a_im, b_re, b_im))

    def to_cells(cos_part, sin_part):
        even = dot3(split_value(cos_part), x_cos(slice(0, half)), NT)
        odd = dot3(split_value(sin_part), x_sin(slice(0, half)), NT)
        both = jnp.concatenate([even + odd, even - odd], 1)
        cos_y = dot3((yih_ref[0], yil_ref[0]), split_value(both[:modes]), NN)
        sin_y = dot3((yih_ref[1], yil_ref[1]), split_value(both[modes:]), NN)
        return cos_y, sin_y

    rows_of = lambda re, im: jnp.concatenate([re, im], 0)
    w_cos, w_sin = to_cells(
        rows_of(jnp.where(live, a_re, 0.0), jnp.where(live, a_im, 0.0)), rows_of(b_re, b_im)
    )
    u_cos, u_sin = to_cells(
        rows_of(-wave_y * pa_im, wave_y * pa_re), rows_of(-wave_y * pb_im, wave_y * pb_re)
    )
    flux_u = ((u_cos * w_cos + u_sin * w_sin), (u_cos * w_sin + u_sin * w_cos))
    v_cos, v_sin = to_cells(
        rows_of(-wave_x * pb_re, -wave_x * pb_im), rows_of(wave_x * pa_re, wave_x * pa_im)
    )
    flux_v = ((v_cos * w_cos + v_sin * w_sin), (v_cos * w_sin + v_sin * w_cos))

    pieces = []
    for flux in (flux_u, flux_v):
        for part in range(2):
            pieces.append(dot3((yoh_ref[own, part], yol_ref[own, part]), split_value(flux[part]), NN))
    hats = jnp.concatenate(pieces, 0)
    hat_cos = dot3(split_value(hats[:, :half] + hats[:, half:]), x_cos(slice(0, half)), NN)
    hat_sin = dot3(split_value(hats[:, :half] - hats[:, half:]), x_sin(slice(0, half)), NN)
    cos1_re, cos1_im, cos2_re, cos2_im = (hat_cos[i * block : (i + 1) * block] for i in range(4))
    sin1_re, sin1_im, sin2_re, sin2_im = (hat_sin[i * block : (i + 1) * block] for i in range(4))

    first = pl.multiple_of(own * block, 8)
    k_lane, wave_x, wave_y, squared = waves(block, first)
    fade = 1.0 - (DT_STEP * VISCOSITY) * squared
    at = pl.ds(first, block)
    new = project(
        plan,
        k_lane,
        coef_ref[0, at, :] * fade - DT_STEP * (wave_x * sin1_re - wave_y * cos2_im),
        coef_ref[1, at, :] * fade - DT_STEP * (wave_x * sin1_im + wave_y * cos2_re),
        coef_ref[2, at, :] * fade - DT_STEP * (-wave_x * cos1_re - wave_y * sin2_im),
        coef_ref[3, at, :] * fade - DT_STEP * (-wave_x * cos1_im + wave_y * sin2_re),
    )
    line = dot3(split_value(rows_of(new[0], new[1])), x_cos(), NT) + dot3(
        split_value(rows_of(new[2], new[3])), x_sin(), NT
    )
    for peer in range(plan.space):
        cut = slice(peer * rows, (peer + 1) * rows)
        out_ref[peer] = jnp.concatenate([line[:block, cut], line[block:, cut]], 1)


def finish_kernel(plan, moved_ref, driving_ref, high_ref, low_ref, out_ref):
    rows, modes, n = plan.rows, plan.modes, plan.n
    ky = lax.broadcasted_iota(jnp.int32, (modes, 2 * rows), 0)
    weight = jnp.where(ky == 0, 1.0 / (n * n), 2.0 / (n * n))
    forcing = DT_STEP * driving_ref[...]
    cos_y = (high_ref[:modes], low_ref[:modes])
    sin_y = (high_ref[modes:], low_ref[modes:])
    for member in range(plan.count):
        line = moved_ref[member * plan.group : (member + 1) * plan.group].reshape(modes, 2 * rows)
        line = jnp.transpose(line * weight)
        fresh = dot3(split_value(line[:rows]), cos_y, NN) + dot3(split_value(line[rows:]), sin_y, NN)
        out_ref[member] = (fresh + forcing).astype(BF16)


def probe_kernel(rows, columns, probes_ref, observed_ref, count_ref, total_ref):
    probes = probes_ref[...]
    observed = observed_ref[...]
    amount = probes.shape[1]
    row, column = lax.div(probes, columns), lax.rem(probes, columns)
    in_row = lax.broadcasted_iota(jnp.int32, (rows, amount), 0) == row
    in_column = (lax.broadcasted_iota(jnp.int32, (columns, amount), 0) == column).astype(F32).astype(BF16)
    first = observed.astype(BF16)
    rest = observed - first.astype(F32)
    second = rest.astype(BF16)
    third = (rest - second.astype(F32)).astype(BF16)
    left = [in_row.astype(F32)]
    left += [jnp.where(in_row, piece.astype(F32), 0.0) for piece in (first, second, third)]
    left = jnp.concatenate(left, 0).astype(BF16)
    out = lax.dot_general(left, in_column, NT, preferred_element_type=F32)
    count_ref[...] = out[:rows]
    total_ref[...] = out[rows : 2 * rows] + (out[2 * rows : 3 * rows] + out[3 * rows :])


def analysis_kernel(count, copies, offset_ref, mixing_ref, values_ref, number_ref, total_ref, out_ref, part_ref, row_ref):
    members, rows, columns = values_ref.shape
    offset = offset_ref[0]
    values = [values_ref[j].astype(F32) for j in range(members)]
    state_sum = values[0]
    for j in range(1, members):
        state_sum = state_sum + values[j]
    for m in range(count):
        weights = [mixing_ref[j, offset + m] for j in range(members)]
        weight_sum = weights[0]
        for j in range(1, members):
            weight_sum = weight_sum + weights[j]
        acc = ((1.0 - weight_sum) * (1.0 / members)) * state_sum
        for j in range(members):
            acc = acc + weights[j] * values[j]
        out_ref[m] = acc
    number = number_ref[...]
    centre = state_sum * (1.0 / members)
    surprise = total_ref[...] - number * centre

    def to_row(product):
        line = jnp.sum(product, 0, keepdims=True)
        short = line[:, :LANES]
        for at in range(LANES, columns, LANES):
            short = short + line[:, at : at + LANES]
        return short

    anomaly = [v - centre for v in values]
    for i in range(members):
        weighted = anomaly[i] * number
        for j in range(i + 1):
            row = to_row(weighted * anomaly[j])
            row_ref[j, pl.ds(i, 1), :] = row
            if j != i:
                row_ref[i, pl.ds(j, 1), :] = row
        row_ref[members, pl.ds(i, 1), :] = to_row(anomaly[i] * surprise)
    lane = lax.broadcasted_iota(jnp.int32, (members, LANES), 1)
    tile = jnp.zeros((members, LANES), F32)
    for j in range(members + 1):
        tile = jnp.where(lane == j, jnp.sum(row_ref[j], 1, keepdims=True), tile)
    for peer in range(copies):
        part_ref[peer] = tile


def total_kernel(probes, parts_ref, spread_ref, projection_ref):
    copies, members, _ = parts_ref.shape
    total = parts_ref[0]
    for s in range(1, copies):
        total = total + parts_ref[s]
    spread_ref[...] = total[:, :members] * (1.0 / probes)
    projection_ref[...] = total[:, members : members + 1] * (1.0 / math.sqrt(probes))


def vmem(count):
    return [pl.BlockSpec(memory_space=pltpu.VMEM)] * count


SMEM = pl.BlockSpec(memory_space=pltpu.SMEM)


def on_device(plan, participant_swirls, driving_source, mixing, probes, observed):
    count, rows, n = participant_swirls.shape
    members, space = mixing.shape[0], plan.space
    own = (lax.axis_index("space") % plan.group).astype(jnp.int32).reshape(1)
    offset = (lax.axis_index("member") * count).astype(jnp.int32).reshape(1)
    y_high, y_low = plan.y_forward

    sent = pl.pallas_call(
        functools.partial(rows_kernel, plan),
        out_shape=jax.ShapeDtypeStruct((space, plan.modes, 2 * rows), F32),
        in_specs=vmem(3),
        out_specs=vmem(1)[0],
        name="rows_to_modes",
    )(participant_swirls.reshape(count * rows, n), y_high, y_low)
    moved = lax.all_to_all(sent, "space", split_axis=0, concat_axis=0, tiled=True)

    number, total = pl.pallas_call(
        functools.partial(probe_kernel, rows, n),
        out_shape=[jax.ShapeDtypeStruct((rows, n), F32)] * 2,
        in_specs=vmem(2),
        out_specs=vmem(2),
        name="probe_cells",
    )(probes.reshape(1, -1), observed.reshape(1, -1))

    line = pl.pallas_call(
        functools.partial(member_kernel, plan),
        out_shape=jax.ShapeDtypeStruct((space, plan.block, 2 * rows), F32),
        in_specs=[SMEM] + vmem(7),
        out_specs=vmem(1)[0],
        scratch_shapes=[pltpu.VMEM((4, plan.modes, plan.kpad), F32)],
        name="member_step",
    )(own, moved, *plan.x_table, *plan.y_inverse, *plan.y_own)
    moved = lax.all_to_all(line, "space", split_axis=0, concat_axis=0, tiled=True)

    rounded = pl.pallas_call(
        functools.partial(finish_kernel, plan),
        out_shape=jax.ShapeDtypeStruct((count, rows, n), BF16),
        in_specs=vmem(4),
        out_specs=vmem(1)[0],
        name="modes_to_rows",
    )(moved, driving_source, y_high, y_low)
    values = lax.all_gather(rounded, "member", axis=0, tiled=True)

    analysis, part = pl.pallas_call(
        functools.partial(analysis_kernel, count, space),
        out_shape=[
            jax.ShapeDtypeStruct((count, rows, n), F32),
            jax.ShapeDtypeStruct((space, members, LANES), F32),
        ],
        in_specs=[SMEM, SMEM] + vmem(3),
        out_specs=vmem(2),
        scratch_shapes=[pltpu.VMEM((members + 1, members, LANES), F32)],
        name="analysis",
    )(offset, mixing, values, number, total)
    parts = lax.all_to_all(part, "space", split_axis=0, concat_axis=0, tiled=True)
    spread, projection = pl.pallas_call(
        functools.partial(total_kernel, probes.shape[0] * space),
        out_shape=[jax.ShapeDtypeStruct((members, members), F32), jax.ShapeDtypeStruct((members, 1), F32)],
        in_specs=vmem(1),
        out_specs=vmem(2),
        name="probe_totals",
    )(parts)
    return analysis, spread, projection.reshape(members)


def solution(mesh):
    space = mesh.shape["space"]

    def body(participant_swirls, *rest):
        count, rows, n = participant_swirls.shape
        return on_device(Plan(n, rows, space, count), participant_swirls, *rest)

    return jax.shard_map(
        body,
        mesh=mesh,
        in_specs=(P("member", "space", None), P("space", None), P(), P("space"), P("space")),
        out_specs=(P("member", "space", None), P(), P()),
        check_vma=False,
    )
```

```python
import functools
import math

import jax
import jax.numpy as jnp
import numpy as np
from jax import lax
from jax.experimental import pallas as pl
from jax.experimental.pallas import tpu as pltpu
from jax.sharding import PartitionSpec as P

KEEP = 160
DT_STEP = 0.1
VISCOSITY = 0.05
LANES = 128
F32 = jnp.float32
BF16 = jnp.bfloat16

NN = (((1,), (0,)), ((), ()))
NT = (((1,), (1,)), ((), ()))
FULL = ((0, 0), (0, 1), (1, 0), (1, 1), (0, 2), (2, 0))
SHORT = ((0, 0), (0, 1), (1, 0))
MIB = 1 << 20


def round_up(value, unit):
    return -(-value // unit) * unit


def split_table(table, pieces):
    rest, out = np.asarray(table, np.float64), []
    for _ in range(pieces):
        out.append(rest.astype(np.float32).astype(BF16))
        rest = rest - out[-1].astype(np.float64)
    return tuple(jnp.asarray(piece) for piece in out)


def split(value, pieces):
    out = []
    for piece in range(pieces):
        out.append(value.astype(BF16))
        if piece + 1 < pieces:
            value = value - out[-1].astype(F32)
    return out


def product(left, right, dims, terms):
    out = None
    for i, j in reversed(terms):
        term = lax.dot_general(left[i], right[j], dims, preferred_element_type=F32)
        out = term if out is None else out + term
    return out


class Plan:
    def __init__(self, n, rows, space, count):
        self.n, self.rows, self.space, self.count = n, rows, space, count
        self.group = space // count
        self.block = round_up(-(-KEEP // self.group), 8)
        self.modes = self.block * self.group
        self.half = n // 2
        self.kpad = round_up(KEEP + 1, LANES)
        cells = np.arange(n) + 0.5
        scale = 2.0 * math.pi / n
        ky = np.arange(self.modes)
        live = (ky < KEEP)[:, None]
        angle_y = scale * ky[:, None] * cells[None, :]
        cos_y, sin_y = np.cos(angle_y) * live, np.sin(angle_y) * live
        self.y_table = split_table(np.concatenate([cos_y, -sin_y], 0), 3)
        own = 2.0 * np.stack([cos_y, -sin_y])[:, :, : self.half]
        own = own.reshape(2, self.group, self.block, self.half).transpose(1, 0, 2, 3)
        self.y_own = split_table(own, 2)
        kx = np.arange(self.kpad)
        angle_x = scale * cells[:, None] * kx[None, :]
        keep_x = (kx <= KEEP)[None, :]
        self.x_table = split_table(np.concatenate([np.cos(angle_x) * keep_x, np.sin(angle_x) * keep_x], 1), 3)


def rows_kernel(plan, field_ref, y0_ref, y1_ref, y2_ref, out_ref):
    rows, modes = plan.rows, plan.modes
    field = split(field_ref[...], 3)
    partial = product((y0_ref[...], y1_ref[...], y2_ref[...]), field, NT, FULL)
    real, imag = partial[:modes], partial[modes:]
    for member in range(plan.count):
        at = slice(member * rows, (member + 1) * rows)
        packed = jnp.concatenate([real[:, at], imag[:, at]], 1)
        for peer in range(plan.group):
            out_ref[member * plan.group + peer] = packed


def project(plan, k_lane, cos_re, cos_im, sin_re, sin_im):
    weight = jnp.where((k_lane == 0) | (k_lane == KEEP), 1.0, 2.0)
    edge = jnp.where(k_lane == KEEP, 1.0, 0.0)
    return (
        weight * cos_re - edge * sin_im,
        weight * cos_im + edge * sin_re,
        weight * sin_re + edge * cos_im,
        weight * sin_im - edge * cos_re,
    )


def member_kernel(plan, own_ref, moved_ref, x0_ref, x1_ref, x2_ref, y0_ref, y1_ref, o0_ref, o1_ref, out_ref):
    n, half, modes, block, kpad, rows = plan.n, plan.half, plan.modes, plan.block, plan.kpad, plan.rows
    unit = 2.0 * math.pi / n
    own = own_ref[0]
    first = pl.multiple_of(own * block, 8)
    x_refs = (x0_ref, x1_ref, x2_ref)

    def x_cos(count, pieces):
        return [ref[:count, :kpad] for ref in x_refs[:pieces]]

    def x_sin(count, pieces):
        return [ref[:count, kpad:] for ref in x_refs[:pieces]]

    def gathered(at):
        real = jnp.concatenate([moved_ref[s, at, :rows] for s in range(plan.space)], 1)
        imag = jnp.concatenate([moved_ref[s, at, rows:] for s in range(plan.space)], 1)
        return jnp.concatenate([real, imag], 0)

    def parts(sums, count):
        return (sums[:count, :kpad], sums[count:, :kpad], sums[:count, kpad:], sums[count:, kpad:])

    def waves(count, start):
        k_lane = lax.broadcasted_iota(jnp.int32, (count, kpad), 1)
        ky_row = lax.broadcasted_iota(jnp.int32, (count, kpad), 0) + start
        wave_x = k_lane.astype(F32) * unit
        wave_y = ky_row.astype(F32) * unit
        return k_lane, ky_row, wave_x, wave_y, wave_x * wave_x + wave_y * wave_y

    x_pair = [x0_ref[...], x1_ref[...]]
    sums = parts(product(split(gathered(slice(0, modes)), 2), x_pair, NN, SHORT), modes)
    k_lane, ky_row, wave_x, wave_y, squared = waves(modes, 0)
    live = squared > 0
    inverse_sq = jnp.where(live, 1.0 / jnp.where(live, squared, 1.0), 0.0)
    weight = jnp.where(ky_row == 0, 1.0 / (n * n), 2.0 / (n * n))
    a_re, a_im, b_re, b_im = project(plan, k_lane, *[s * weight for s in sums])
    pa_re, pa_im, pb_re, pb_im = (c * inverse_sq for c in (a_re, a_im, b_re, b_im))
    y_cos = [jnp.transpose(ref[:modes, :half].astype(F32)).astype(BF16) for ref in (y0_ref, y1_ref)]
    y_sin = [jnp.transpose(ref[modes:, :half].astype(F32)).astype(BF16) for ref in (y0_ref, y1_ref)]

    def to_cells(cos_part, sin_part):
        even = product(split(cos_part, 2), x_cos(half, 2), NT, SHORT)
        odd = product(split(sin_part, 2), x_sin(half, 2), NT, SHORT)
        both = jnp.concatenate([even + odd, even - odd], 1)
        cos_y = product(y_cos, split(both[:modes], 2), NN, SHORT)
        sin_y = product(y_sin, split(both[modes:], 2), NN, SHORT)
        return cos_y, sin_y

    rows_of = lambda re, im: jnp.concatenate([re, im], 0)
    w_cos, w_sin = to_cells(
        rows_of(jnp.where(live, a_re, 0.0), jnp.where(live, a_im, 0.0)), rows_of(b_re, b_im)
    )
    u_cos, u_sin = to_cells(
        rows_of(-wave_y * pa_im, wave_y * pa_re), rows_of(-wave_y * pb_im, wave_y * pb_re)
    )
    flux_u = (u_cos * w_cos + u_sin * w_sin, u_cos * w_sin + u_sin * w_cos)
    v_cos, v_sin = to_cells(
        rows_of(-wave_x * pb_re, -wave_x * pb_im), rows_of(wave_x * pa_re, wave_x * pa_im)
    )
    flux_v = (v_cos * w_cos + v_sin * w_sin, v_cos * w_sin + v_sin * w_cos)

    pieces = []
    for flux in (flux_u, flux_v):
        for part in range(2):
            pieces.append(product((o0_ref[own, part], o1_ref[own, part]), split(flux[part], 2), NN, SHORT))
    hats = jnp.concatenate(pieces, 0)
    hat_cos = product(split(hats[:, :half] + hats[:, half:], 2), x_cos(half, 2), NN, SHORT)
    hat_sin = product(split(hats[:, :half] - hats[:, half:], 2), x_sin(half, 2), NN, SHORT)
    cos1_re, cos1_im, cos2_re, cos2_im = (hat_cos[i * block : (i + 1) * block] for i in range(4))
    sin1_re, sin1_im, sin2_re, sin2_im = (hat_sin[i * block : (i + 1) * block] for i in range(4))

    mine = product(split(gathered(pl.ds(first, block)), 3), [ref[...] for ref in x_refs], NN, FULL)
    mine = parts(mine, block)
    k_lane, _, wave_x, wave_y, squared = waves(block, first)
    fade = 1.0 - (DT_STEP * VISCOSITY) * squared
    new = project(
        plan,
        k_lane,
        mine[0] * fade - DT_STEP * (wave_x * sin1_re - wave_y * cos2_im),
        mine[1] * fade - DT_STEP * (wave_x * sin1_im + wave_y * cos2_re),
        mine[2] * fade - DT_STEP * (-wave_x * cos1_re - wave_y * sin2_im),
        mine[3] * fade - DT_STEP * (-wave_x * cos1_im + wave_y * sin2_re),
    )
    line = product(split(rows_of(new[0], new[1]), 3), x_cos(n, 3), NT, FULL) + product(
        split(rows_of(new[2], new[3]), 3), x_sin(n, 3), NT, FULL
    )
    for peer in range(plan.space):
        cut = slice(peer * rows, (peer + 1) * rows)
        out_ref[peer] = jnp.concatenate([line[:block, cut], line[block:, cut]], 1)


def finish_kernel(plan, moved_ref, driving_ref, y0_ref, y1_ref, y2_ref, out_ref):
    rows, modes, n, count = plan.rows, plan.modes, plan.n, plan.count
    ky = lax.broadcasted_iota(jnp.int32, (modes, 2 * rows), 0)
    weight = jnp.where(ky == 0, 1.0 / (n * n), 2.0 / (n * n))
    lines = []
    for member in range(count):
        line = moved_ref[member * plan.group : (member + 1) * plan.group].reshape(modes, 2 * rows)
        lines.append(jnp.transpose(line * weight))
    real = jnp.concatenate([line[:rows] for line in lines], 0)
    imag = jnp.concatenate([line[rows:] for line in lines], 0)
    y_refs = (y0_ref, y1_ref, y2_ref)
    fresh = product(split(real, 3), [ref[:modes] for ref in y_refs], NN, FULL)
    fresh = fresh + product(split(imag, 3), [ref[modes:] for ref in y_refs], NN, FULL)
    forcing = DT_STEP * driving_ref[...]
    for member in range(count):
        out_ref[member] = (fresh[member * rows : (member + 1) * rows] + forcing).astype(BF16)


def probe_kernel(rows, columns, probes_ref, observed_ref, count_ref, total_ref):
    probes = probes_ref[...]
    observed = observed_ref[...]
    amount = probes.shape[1]
    row, column = lax.div(probes, columns), lax.rem(probes, columns)
    in_row = lax.broadcasted_iota(jnp.int32, (rows, amount), 0) == row
    in_column = (lax.broadcasted_iota(jnp.int32, (columns, amount), 0) == column).astype(F32).astype(BF16)
    first = observed.astype(BF16)
    rest = observed - first.astype(F32)
    second = rest.astype(BF16)
    third = (rest - second.astype(F32)).astype(BF16)
    left = [in_row.astype(F32)]
    left += [jnp.where(in_row, piece.astype(F32), 0.0) for piece in (first, second, third)]
    left = jnp.concatenate(left, 0).astype(BF16)
    out = lax.dot_general(left, in_column, NT, preferred_element_type=F32)
    count_ref[...] = out[:rows]
    total_ref[...] = out[rows : 2 * rows] + (out[2 * rows : 3 * rows] + out[3 * rows :])


def state_sum_of(values):
    total = values[0]
    for value in values[1:]:
        total = total + value
    return total


def analysis_kernel(count, offset_ref, mixing_ref, values_ref, out_ref):
    members = values_ref.shape[0]
    offset = offset_ref[0]
    values = [values_ref[j].astype(F32) for j in range(members)]
    state_sum = state_sum_of(values)
    for m in range(count):
        weights = [mixing_ref[j, offset + m] for j in range(members)]
        acc = ((1.0 - state_sum_of(weights)) * (1.0 / members)) * state_sum
        for j in range(members):
            acc = acc + weights[j] * values[j]
        out_ref[m] = acc


def products_kernel(copies, values_ref, number_ref, total_ref, part_ref, row_ref):
    members, rows, columns = values_ref.shape
    values = [values_ref[j].astype(F32) for j in range(members)]
    number = number_ref[...]
    centre = state_sum_of(values) * (1.0 / members)
    surprise = total_ref[...] - number * centre

    def to_row(product):
        line = jnp.sum(product, 0, keepdims=True)
        short = line[:, :LANES]
        for at in range(LANES, columns, LANES):
            short = short + line[:, at : at + LANES]
        return short

    anomaly = [v - centre for v in values]
    for i in range(members):
        weighted = anomaly[i] * number
        for j in range(i + 1):
            row = to_row(weighted * anomaly[j])
            row_ref[j, pl.ds(i, 1), :] = row
            if j != i:
                row_ref[i, pl.ds(j, 1), :] = row
        row_ref[members, pl.ds(i, 1), :] = to_row(anomaly[i] * surprise)
    lane = lax.broadcasted_iota(jnp.int32, (members, LANES), 1)
    tile = jnp.zeros((members, LANES), F32)
    for j in range(members + 1):
        tile = jnp.where(lane == j, jnp.sum(row_ref[j], 1, keepdims=True), tile)
    for peer in range(copies):
        part_ref[peer] = tile


def total_kernel(probes, parts_ref, spread_ref, projection_ref):
    copies, members, lanes = parts_ref.shape
    total = parts_ref[0]
    for s in range(1, copies):
        total = total + parts_ref[s]
    spread_ref[...] = total[:, :members] * (1.0 / probes)
    lane = lax.broadcasted_iota(jnp.int32, (members, lanes), 1)
    row = lax.broadcasted_iota(jnp.int32, (members, lanes), 0)
    column = jnp.where(lane == row, total[:, members : members + 1], 0.0)
    projection_ref[...] = jnp.sum(column, 0, keepdims=True)[:, :members] * (1.0 / math.sqrt(probes))


VMEM = pl.BlockSpec(memory_space=pltpu.VMEM)
SMEM = pl.BlockSpec(memory_space=pltpu.SMEM)


def local(kernel, name, limit, in_specs, out_shape, scratch=()):
    return pl.pallas_call(
        kernel,
        out_shape=out_shape,
        in_specs=in_specs,
        out_specs=jax.tree.map(lambda _: VMEM, out_shape),
        scratch_shapes=scratch,
        compiler_params=pltpu.CompilerParams(vmem_limit_bytes=limit * MIB),
        name=name,
    )


def on_device(plan, participant_swirls, driving_source, mixing, probes, observed):
    count, rows, n = participant_swirls.shape
    members, space = mixing.shape[0], plan.space
    array = jax.ShapeDtypeStruct
    own = (lax.axis_index("space") % plan.group).astype(jnp.int32).reshape(1)
    offset = (lax.axis_index("member") * count).astype(jnp.int32).reshape(1)
    exchange = functools.partial(lax.all_to_all, axis_name="space", split_axis=0, concat_axis=0, tiled=True)

    sent = local(
        functools.partial(rows_kernel, plan), "rows_to_modes", 8, [VMEM] * 4,
        array((space, plan.modes, 2 * rows), F32),
    )(participant_swirls.reshape(count * rows, n), *plan.y_table)
    moved = exchange(sent)
    number, total = local(
        functools.partial(probe_kernel, rows, n), "probe_cells", 16, [VMEM] * 2, [array((rows, n), F32)] * 2
    )(probes.reshape(1, -1), observed.reshape(1, -1))
    line = local(
        functools.partial(member_kernel, plan), "member_step", 24, [SMEM] + [VMEM] * 8,
        array((space, plan.block, 2 * rows), F32),
    )(own, moved, *plan.x_table, *plan.y_table[:2], *plan.y_own)
    moved = exchange(line)
    rounded = local(
        functools.partial(finish_kernel, plan), "modes_to_rows", 8, [VMEM] * 5, array((count, rows, n), BF16)
    )(moved, driving_source, *plan.y_table)
    values = lax.all_gather(rounded, "member", axis=0, tiled=True)
    part = local(
        functools.partial(products_kernel, space), "products", 16, [VMEM] * 3,
        array((space, members, LANES), F32),
        [pltpu.VMEM((members + 1, members, LANES), F32)],
    )(values, number, total)
    parts = exchange(part)
    analysis = local(
        functools.partial(analysis_kernel, count), "analysis", 16, [SMEM, SMEM, VMEM], array((count, rows, n), F32)
    )(offset, mixing, values)
    spread, projection = local(
        functools.partial(total_kernel, probes.shape[0] * space), "probe_totals", 4, [VMEM],
        [array((members, members), F32), array((1, members), F32)],
    )(parts)
    return analysis, spread, projection.reshape(members)


def solution(mesh):
    space = mesh.shape["space"]

    def body(participant_swirls, *rest):
        count, rows, n = participant_swirls.shape
        return on_device(Plan(n, rows, space, count), participant_swirls, *rest)

    return jax.shard_map(
        body,
        mesh=mesh,
        in_specs=(P("member", "space", None), P("space", None), P(), P("space"), P("space")),
        out_specs=(P("member", "space", None), P(), P()),
        check_vma=False,
    )
```

```python
import functools
import math

import jax
import jax.numpy as jnp
import numpy as np
from jax import lax
from jax.experimental import pallas as pl
from jax.experimental.pallas import tpu as pltpu
from jax.sharding import PartitionSpec as P

KEEP = 160
DT_STEP = 0.1
VISCOSITY = 0.05
LANES = 128
F32 = jnp.float32
BF16 = jnp.bfloat16

NN = (((1,), (0,)), ((), ()))
NT = (((1,), (1,)), ((), ()))
FULL = ((0, 0), (0, 1), (1, 0), (1, 1), (0, 2), (2, 0))
SHORT = ((0, 0), (0, 1), (1, 0))
MIB = 1 << 20


def round_up(value, unit):
    return -(-value // unit) * unit


def split_table(table, pieces):
    rest, out = np.asarray(table, np.float64), []
    for _ in range(pieces):
        out.append(rest.astype(np.float32).astype(BF16))
        rest = rest - out[-1].astype(np.float64)
    return tuple(jnp.asarray(piece) for piece in out)


def split(value, pieces):
    out = []
    for piece in range(pieces):
        out.append(value.astype(BF16))
        if piece + 1 < pieces:
            value = value - out[-1].astype(F32)
    return out


def product(left, right, dims, terms):
    out = None
    for i, j in reversed(terms):
        term = lax.dot_general(left[i], right[j], dims, preferred_element_type=F32)
        out = term if out is None else out + term
    return out


class Plan:
    def __init__(self, n, rows, space, count):
        self.n, self.rows, self.space, self.count = n, rows, space, count
        self.group = space // count
        self.block = round_up(-(-KEEP // self.group), 8)
        self.modes = self.block * self.group
        self.half = n // 2
        self.kpad = round_up(KEEP + 1, LANES)
        cells = np.arange(n) + 0.5
        scale = 2.0 * math.pi / n
        ky = np.arange(self.modes)
        live = (ky < KEEP)[:, None]
        angle_y = scale * ky[:, None] * cells[None, :]
        cos_y, sin_y = np.cos(angle_y) * live, np.sin(angle_y) * live
        self.y_table = split_table(np.concatenate([cos_y, -sin_y], 0), 3)
        own = 2.0 * np.stack([cos_y, -sin_y])[:, :, : self.half]
        own = own.reshape(2, self.group, self.block, self.half).transpose(1, 0, 2, 3)
        self.y_own = split_table(own, 2)
        kx = np.arange(self.kpad)
        angle_x = scale * cells[:, None] * kx[None, :]
        keep_x = (kx <= KEEP)[None, :]
        self.x_table = split_table(np.concatenate([np.cos(angle_x) * keep_x, np.sin(angle_x) * keep_x], 1), 3)


def rows_kernel(plan, me_ref, field_hbm, y0_hbm, y1_hbm, y2_hbm, *refs):
    rows, modes, count = plan.rows, plan.modes, plan.count
    outs, (field_ref, y0_ref, y1_ref, y2_ref, packed_ref, sems) = refs[:count], refs[count:]
    sources = (field_hbm, y0_hbm, y1_hbm, y2_hbm)
    copies = [
        pltpu.make_async_copy(source, target, sems.at[i])
        for i, (source, target) in enumerate(zip(sources, (field_ref, y0_ref, y1_ref, y2_ref)))
    ]
    for copy in copies:
        copy.start()
    for copy in copies:
        copy.wait()
    field = split(field_ref[...], 3)
    partial = product((y0_ref[...], y1_ref[...], y2_ref[...]), field, NT, FULL)
    real, imag = partial[:modes], partial[modes:]
    for member in range(count):
        at = slice(member * rows, (member + 1) * rows)
        packed_ref[member] = jnp.concatenate([real[:, at], imag[:, at]], 1)
    side = me_ref[0] // plan.group
    for away in range(count):
        outs[away][...] = packed_ref[side ^ away]


def project(plan, k_lane, cos_re, cos_im, sin_re, sin_im):
    weight = jnp.where((k_lane == 0) | (k_lane == KEEP), 1.0, 2.0)
    edge = jnp.where(k_lane == KEEP, 1.0, 0.0)
    return (
        weight * cos_re - edge * sin_im,
        weight * cos_im + edge * sin_re,
        weight * sin_re + edge * cos_im,
        weight * sin_im - edge * cos_re,
    )


def member_kernel(plan, me_ref, x0_ref, x1_ref, x2_ref, y0_ref, y1_ref, o0_ref, o1_ref, *refs):
    blocks, out_ref, moved_ref = refs[: plan.space], refs[plan.space], refs[plan.space + 1]
    me = me_ref[0]
    for away in range(plan.space):
        moved_ref[me ^ away] = blocks[away][...]
    n, half, modes, block, kpad, rows = plan.n, plan.half, plan.modes, plan.block, plan.kpad, plan.rows
    unit = 2.0 * math.pi / n
    own = me % plan.group
    first = pl.multiple_of(own * block, 8)
    x_refs = (x0_ref, x1_ref, x2_ref)

    def x_cos(count, pieces):
        return [ref[:count, :kpad] for ref in x_refs[:pieces]]

    def x_sin(count, pieces):
        return [ref[:count, kpad:] for ref in x_refs[:pieces]]

    def gathered(at):
        real = jnp.concatenate([moved_ref[s, at, :rows] for s in range(plan.space)], 1)
        imag = jnp.concatenate([moved_ref[s, at, rows:] for s in range(plan.space)], 1)
        return jnp.concatenate([real, imag], 0)

    def parts(sums, count):
        return (sums[:count, :kpad], sums[count:, :kpad], sums[:count, kpad:], sums[count:, kpad:])

    def waves(count, start):
        k_lane = lax.broadcasted_iota(jnp.int32, (count, kpad), 1)
        ky_row = lax.broadcasted_iota(jnp.int32, (count, kpad), 0) + start
        wave_x = k_lane.astype(F32) * unit
        wave_y = ky_row.astype(F32) * unit
        return k_lane, ky_row, wave_x, wave_y, wave_x * wave_x + wave_y * wave_y

    x_pair = [x0_ref[...], x1_ref[...]]
    sums = parts(product(split(gathered(slice(0, modes)), 2), x_pair, NN, SHORT), modes)
    k_lane, ky_row, wave_x, wave_y, squared = waves(modes, 0)
    live = squared > 0
    inverse_sq = jnp.where(live, 1.0 / jnp.where(live, squared, 1.0), 0.0)
    weight = jnp.where(ky_row == 0, 1.0 / (n * n), 2.0 / (n * n))
    a_re, a_im, b_re, b_im = project(plan, k_lane, *[s * weight for s in sums])
    pa_re, pa_im, pb_re, pb_im = (c * inverse_sq for c in (a_re, a_im, b_re, b_im))
    y_cos = [jnp.transpose(ref[:modes, :half].astype(F32)).astype(BF16) for ref in (y0_ref, y1_ref)]
    y_sin = [jnp.transpose(ref[modes:, :half].astype(F32)).astype(BF16) for ref in (y0_ref, y1_ref)]

    def to_cells(cos_part, sin_part):
        even = product(split(cos_part, 2), x_cos(half, 2), NT, SHORT)
        odd = product(split(sin_part, 2), x_sin(half, 2), NT, SHORT)
        both = jnp.concatenate([even + odd, even - odd], 1)
        cos_y = product(y_cos, split(both[:modes], 2), NN, SHORT)
        sin_y = product(y_sin, split(both[modes:], 2), NN, SHORT)
        return cos_y, sin_y

    rows_of = lambda re, im: jnp.concatenate([re, im], 0)
    def along_x(cos_re, cos_im, sin_re, sin_im):
        return to_cells(
            rows_of(wave_x * sin_re, wave_x * sin_im), rows_of(-wave_x * cos_re, -wave_x * cos_im)
        )

    def along_y(cos_re, cos_im, sin_re, sin_im):
        return to_cells(
            rows_of(-wave_y * cos_im, wave_y * cos_re), rows_of(-wave_y * sin_im, wave_y * sin_re)
        )

    w_modes, p_modes = (a_re, a_im, b_re, b_im), (pa_re, pa_im, pb_re, pb_im)
    u_cos, u_sin = along_y(*p_modes)
    w_cos, w_sin = along_x(*w_modes)
    even = u_cos * w_cos + u_sin * w_sin
    odd = u_cos * w_sin + u_sin * w_cos
    v_cos, v_sin = along_x(*p_modes)
    w_cos, w_sin = along_y(*w_modes)
    even = even - (v_cos * w_cos + v_sin * w_sin)
    odd = odd - (v_cos * w_sin + v_sin * w_cos)

    hats = rows_of(
        product((o0_ref[own, 0], o1_ref[own, 0]), split(even, 2), NN, SHORT),
        product((o0_ref[own, 1], o1_ref[own, 1]), split(odd, 2), NN, SHORT),
    )
    hat_cos = product(split(hats[:, :half] + hats[:, half:], 2), x_cos(half, 2), NN, SHORT)
    hat_sin = product(split(hats[:, :half] - hats[:, half:], 2), x_sin(half, 2), NN, SHORT)
    advect = (hat_cos[:block], hat_cos[block:], hat_sin[:block], hat_sin[block:])

    mine = product(split(gathered(pl.ds(first, block)), 3), [ref[...] for ref in x_refs], NN, FULL)
    mine = parts(mine, block)
    k_lane, _, _, _, squared = waves(block, first)
    fade = 1.0 - (DT_STEP * VISCOSITY) * squared
    new = project(plan, k_lane, *[m * fade - DT_STEP * q for m, q in zip(mine, advect)])
    line = product(split(rows_of(new[0], new[1]), 3), x_cos(n, 3), NT, FULL) + product(
        split(rows_of(new[2], new[3]), 3), x_sin(n, 3), NT, FULL
    )
    for peer in range(plan.space):
        cut = slice(peer * rows, (peer + 1) * rows)
        out_ref[peer] = jnp.concatenate([line[:block, cut], line[block:, cut]], 1)


def finish_kernel(plan, moved_ref, driving_ref, y0_ref, y1_ref, y2_ref, out_ref):
    rows, modes, n, count = plan.rows, plan.modes, plan.n, plan.count
    ky = lax.broadcasted_iota(jnp.int32, (modes, 2 * rows), 0)
    weight = jnp.where(ky == 0, 1.0 / (n * n), 2.0 / (n * n))
    lines = []
    for member in range(count):
        line = moved_ref[member * plan.group : (member + 1) * plan.group].reshape(modes, 2 * rows)
        lines.append(jnp.transpose(line * weight))
    real = jnp.concatenate([line[:rows] for line in lines], 0)
    imag = jnp.concatenate([line[rows:] for line in lines], 0)
    y_refs = (y0_ref, y1_ref, y2_ref)
    fresh = product(split(real, 3), [ref[:modes] for ref in y_refs], NN, FULL)
    fresh = fresh + product(split(imag, 3), [ref[modes:] for ref in y_refs], NN, FULL)
    forcing = DT_STEP * driving_ref[...]
    for member in range(count):
        out_ref[member] = (fresh[member * rows : (member + 1) * rows] + forcing).astype(BF16)


def probe_kernel(rows, columns, probes_ref, observed_ref, count_ref, total_ref):
    probes = probes_ref[...]
    observed = observed_ref[...]
    amount = probes.shape[1]
    row, column = lax.div(probes, columns), lax.rem(probes, columns)
    in_row = lax.broadcasted_iota(jnp.int32, (rows, amount), 0) == row
    in_column = (lax.broadcasted_iota(jnp.int32, (columns, amount), 0) == column).astype(F32).astype(BF16)
    first = observed.astype(BF16)
    rest = observed - first.astype(F32)
    second = rest.astype(BF16)
    third = (rest - second.astype(F32)).astype(BF16)
    left = [in_row.astype(F32)]
    left += [jnp.where(in_row, piece.astype(F32), 0.0) for piece in (first, second, third)]
    left = jnp.concatenate(left, 0).astype(BF16)
    out = lax.dot_general(left, in_column, NT, preferred_element_type=F32)
    count_ref[...] = out[:rows]
    total_ref[...] = out[rows : 2 * rows] + (out[2 * rows : 3 * rows] + out[3 * rows :])


def state_sum_of(values):
    total = values[0]
    for value in values[1:]:
        total = total + value
    return total


def analysis_kernel(count, offset_ref, mixing_ref, values_ref, out_ref):
    members = values_ref.shape[0]
    offset = offset_ref[0]
    values = [values_ref[j].astype(F32) for j in range(members)]
    state_sum = state_sum_of(values)
    for m in range(count):
        weights = [mixing_ref[j, offset + m] for j in range(members)]
        acc = ((1.0 - state_sum_of(weights)) * (1.0 / members)) * state_sum
        for j in range(members):
            acc = acc + weights[j] * values[j]
        out_ref[m] = acc


def products_kernel(values_ref, number_ref, total_ref, part_ref, row_ref):
    members, rows, columns = values_ref.shape
    values = [values_ref[j].astype(F32) for j in range(members)]
    number = number_ref[...]
    centre = state_sum_of(values) * (1.0 / members)
    surprise = total_ref[...] - number * centre

    def to_row(product):
        line = jnp.sum(product, 0, keepdims=True)
        short = line[:, :LANES]
        for at in range(LANES, columns, LANES):
            short = short + line[:, at : at + LANES]
        return short

    anomaly = [v - centre for v in values]
    for i in range(members):
        weighted = anomaly[i] * number
        for j in range(i + 1):
            row = to_row(weighted * anomaly[j])
            row_ref[j, pl.ds(i, 1), :] = row
            if j != i:
                row_ref[i, pl.ds(j, 1), :] = row
        row_ref[members, pl.ds(i, 1), :] = to_row(anomaly[i] * surprise)
    lane = lax.broadcasted_iota(jnp.int32, (members, LANES), 1)
    tile = jnp.zeros((members, LANES), F32)
    for j in range(members + 1):
        tile = jnp.where(lane == j, jnp.sum(row_ref[j], 1, keepdims=True), tile)
    part_ref[...] = tile


def tree_sum(parts):
    while len(parts) > 1:
        parts = [a + b for a, b in zip(parts[::2], parts[1::2])]
    return parts[0]


def sum_kernel(*refs):
    refs[-1][...] = tree_sum([ref[...] for ref in refs[:-1]])


def total_kernel(probes, *refs):
    spread_ref, projection_ref = refs[-2:]
    total = tree_sum([ref[...] for ref in refs[:-2]])
    members, lanes = total.shape
    spread_ref[...] = total[:, :members] * (1.0 / probes)
    lane = lax.broadcasted_iota(jnp.int32, (members, lanes), 1)
    row = lax.broadcasted_iota(jnp.int32, (members, lanes), 0)
    column = jnp.where(lane == row, total[:, members : members + 1], 0.0)
    projection_ref[...] = jnp.sum(column, 0, keepdims=True)[:, :members] * (1.0 / math.sqrt(probes))


VMEM = pl.BlockSpec(memory_space=pltpu.VMEM)
SMEM = pl.BlockSpec(memory_space=pltpu.SMEM)
HBM = pl.BlockSpec(memory_space=pltpu.HBM)


def local(kernel, name, limit, in_specs, out_shape, scratch=()):
    return pl.pallas_call(
        kernel,
        out_shape=out_shape,
        in_specs=in_specs,
        out_specs=jax.tree.map(lambda _: VMEM, out_shape),
        scratch_shapes=scratch,
        compiler_params=pltpu.CompilerParams(vmem_limit_bytes=limit * MIB),
        name=name,
    )


def on_device(plan, participant_swirls, driving_source, mixing, probes, observed):
    count, rows, n = participant_swirls.shape
    members, space = mixing.shape[0], plan.space
    array = jax.ShapeDtypeStruct
    me = lax.axis_index("space").astype(jnp.int32).reshape(1)
    offset = (lax.axis_index("member") * count).astype(jnp.int32).reshape(1)
    group = plan.group

    def from_peer(value, away):
        return lax.ppermute(value, "space", [(d, d ^ away) for d in range(space)])

    block_shape = (plan.modes, 2 * rows)
    table = pltpu.VMEM((2 * plan.modes, n), BF16)
    sent = local(
        functools.partial(rows_kernel, plan), "rows_to_modes", 8, [SMEM] + [HBM] * 4,
        [array(block_shape, F32)] * count,
        [pltpu.VMEM((count * rows, n), F32), table, table, table,
         pltpu.VMEM((count,) + block_shape, F32), pltpu.SemaphoreType.DMA((4,))],
    )(me, *[pltpu.with_memory_space_constraint(x, pltpu.HBM)
            for x in (participant_swirls.reshape(count * rows, n), *plan.y_table)])
    blocks = []
    for side in range(count):
        base = sent[0] if side == 0 else from_peer(sent[side], side * group)
        blocks += [base] + [from_peer(base, away) for away in range(1, group)]
    number, total = local(
        functools.partial(probe_kernel, rows, n), "probe_cells", 16, [VMEM] * 2, [array((rows, n), F32)] * 2
    )(probes.reshape(1, -1), observed.reshape(1, -1))
    line = local(
        functools.partial(member_kernel, plan), "member_step", 24, [SMEM] + [VMEM] * (7 + space),
        array((space, plan.block, 2 * rows), F32),
        [pltpu.VMEM((space,) + block_shape, F32)],
    )(me, *plan.x_table, *plan.y_table[:2], *plan.y_own, *blocks)
    moved = lax.all_to_all(line, "space", split_axis=0, concat_axis=0, tiled=True)
    rounded = local(
        functools.partial(finish_kernel, plan), "modes_to_rows", 8, [VMEM] * 5, array((count, rows, n), BF16)
    )(moved, driving_source, *plan.y_table)
    values = lax.all_gather(rounded, "member", axis=0, tiled=True)
    tile = array((members, LANES), F32)
    part = local(
        products_kernel, "products", 16, [VMEM] * 3, tile, [pltpu.VMEM((members + 1, members, LANES), F32)]
    )(values, number, total)
    part = local(sum_kernel, "side_sum", 4, [VMEM] * group, tile)(
        part, *[from_peer(part, away) for away in range(1, group)]
    )
    analysis = local(
        functools.partial(analysis_kernel, count), "analysis", 16, [SMEM, SMEM, VMEM], array((count, rows, n), F32)
    )(offset, mixing, values)
    spread, projection = local(
        functools.partial(total_kernel, probes.shape[0] * space), "probe_totals", 4, [VMEM] * count,
        [array((members, members), F32), array((1, members), F32)],
    )(part, *[from_peer(part, side * group) for side in range(1, count)])
    return analysis, spread, projection.reshape(members)


def solution(mesh):
    space = mesh.shape["space"]

    def body(participant_swirls, *rest):
        count, rows, n = participant_swirls.shape
        return on_device(Plan(n, rows, space, count), participant_swirls, *rest)

    return jax.shard_map(
        body,
        mesh=mesh,
        in_specs=(P("member", "space", None), P("space", None), P(), P("space"), P("space")),
        out_specs=(P("member", "space", None), P(), P()),
        check_vma=False,
    )
```

```python
import functools
import math

import jax
import jax.numpy as jnp
import numpy as np
from jax import lax
from jax.experimental import pallas as pl
from jax.experimental.pallas import tpu as pltpu
from jax.sharding import PartitionSpec as P

KEEP = 160
DT_STEP = 0.1
VISCOSITY = 0.05
LANES = 128
F32 = jnp.float32
BF16 = jnp.bfloat16

NN = (((1,), (0,)), ((), ()))
NT = (((1,), (1,)), ((), ()))
FULL = ((0, 0), (0, 1), (1, 0), (1, 1), (0, 2), (2, 0))
SHORT = ((0, 0), (0, 1), (1, 0))
MIB = 1 << 20


def round_up(value, unit):
    return -(-value // unit) * unit


def split_table(table, pieces):
    rest, out = np.asarray(table, np.float64), []
    for _ in range(pieces):
        out.append(rest.astype(np.float32).astype(BF16))
        rest = rest - out[-1].astype(np.float64)
    return tuple(jnp.asarray(piece) for piece in out)


def split(value, pieces):
    out = []
    for piece in range(pieces):
        out.append(value.astype(BF16))
        if piece + 1 < pieces:
            value = value - out[-1].astype(F32)
    return out


def product(left, right, dims, terms):
    out = None
    for i, j in reversed(terms):
        term = lax.dot_general(left[i], right[j], dims, preferred_element_type=F32)
        out = term if out is None else out + term
    return out


class Plan:
    def __init__(self, n, rows, space, count):
        self.n, self.rows, self.space, self.count = n, rows, space, count
        self.group = space // count
        self.block = round_up(-(-KEEP // self.group), 8)
        self.modes = self.block * self.group
        self.half = n // 2
        self.kpad = round_up(KEEP + 1, LANES)
        cells = np.arange(n) + 0.5
        scale = 2.0 * math.pi / n
        ky = np.concatenate([np.arange(0, self.modes, 2), np.arange(1, self.modes, 2)])
        live = (ky < KEEP)[:, None]
        angle_y = scale * ky[:, None] * cells[None, :]
        waves_y = np.stack([np.cos(angle_y) * live, -np.sin(angle_y) * live])
        self.y_table = split_table(waves_y.reshape(2 * self.modes, n), 3)
        quarter = waves_y[:, :, : n // 4]
        self.quarter = n // 4
        high, low = split_table(quarter.reshape(2, 2, self.modes // 2, n // 4).transpose(0, 1, 3, 2), 2)
        self.y_inverse = jnp.concatenate([high, high, low], -1)
        own = 2.0 * quarter.reshape(2, self.group, self.block, n // 4).transpose(1, 0, 2, 3)
        high, low = split_table(own, 2)
        self.y_own = jnp.concatenate(
            [jnp.concatenate([high, high], -1), jnp.concatenate([low, jnp.zeros_like(low)], -1)], -2
        )
        kx = np.arange(self.kpad)
        angle_x = scale * cells[: self.half, None] * kx[None, :]
        keep_x = (kx <= KEEP)[None, :]
        self.x_table = split_table(np.concatenate([np.cos(angle_x) * keep_x, np.sin(angle_x) * keep_x], 1), 3)


def rows_kernel(plan, me_ref, field_hbm, y0_hbm, y1_hbm, y2_hbm, *refs):
    rows, modes, count = plan.rows, plan.modes, plan.count
    outs, (field_ref, y0_ref, y1_ref, y2_ref, packed_ref, sems) = refs[:count], refs[count:]
    sources = (field_hbm, y0_hbm, y1_hbm, y2_hbm)
    copies = [
        pltpu.make_async_copy(source, target, sems.at[i])
        for i, (source, target) in enumerate(zip(sources, (field_ref, y0_ref, y1_ref, y2_ref)))
    ]
    for copy in copies:
        copy.start()
    for copy in copies:
        copy.wait()
    field = split(field_ref[...], 3)
    partial = product((y0_ref[...], y1_ref[...], y2_ref[...]), field, NT, FULL)
    real, imag = partial[:modes], partial[modes:]
    for member in range(count):
        at = slice(member * rows, (member + 1) * rows)
        packed_ref[member] = jnp.concatenate([real[:, at], imag[:, at]], 1)
    side = me_ref[0] // plan.group
    for away in range(count):
        outs[away][...] = packed_ref[side ^ away]


def project(plan, k_lane, cos_re, cos_im, sin_re, sin_im):
    weight = jnp.where((k_lane == 0) | (k_lane == KEEP), 1.0, 2.0)
    edge = jnp.where(k_lane == KEEP, 1.0, 0.0)
    return (
        weight * cos_re - edge * sin_im,
        weight * cos_im + edge * sin_re,
        weight * sin_re + edge * cos_im,
        weight * sin_im - edge * cos_re,
    )


def member_kernel(plan, me_ref, x0_hbm, x1_hbm, x2_hbm, inverse_hbm, own_hbm, *refs):
    blocks, out_ref, moved_ref = refs[: plan.space], refs[plan.space], refs[plan.space + 1]
    x0_ref, x1_ref, x2_ref, inverse_ref, own_ref, coef_ref, sems = refs[plan.space + 2 :]
    me = me_ref[0]
    own = me % plan.group
    copies = [
        pltpu.make_async_copy(source, target, sems.at[i])
        for i, (source, target) in enumerate(
            [(x0_hbm, x0_ref), (x1_hbm, x1_ref), (x2_hbm, x2_ref), (inverse_hbm, inverse_ref), (own_hbm.at[own], own_ref)]
        )
    ]
    for copy in copies:
        copy.start()
    for away in range(plan.space):
        moved_ref[me ^ away] = blocks[away][...]
    n, half, modes, block, kpad, rows = plan.n, plan.half, plan.modes, plan.block, plan.kpad, plan.rows
    unit = 2.0 * math.pi / n
    first = pl.multiple_of(own * block, 8)
    x_refs = (x0_ref, x1_ref, x2_ref)

    def x_cos(pieces):
        return [ref[:, :kpad] for ref in x_refs[:pieces]]

    def x_sin(pieces):
        return [ref[:, kpad:] for ref in x_refs[:pieces]]

    swap = lax.broadcasted_iota(jnp.int32, (half, half), 0) + lax.broadcasted_iota(jnp.int32, (half, half), 1)
    swap = jnp.where(swap == half - 1, 1.0, 0.0).astype(BF16)

    def reversed_lanes(value):
        return product(split(value, 3), [swap], NN, ((0, 0), (1, 0), (2, 0)))

    def gathered(lanes, first, last):
        return jnp.concatenate([moved_ref[s, :, lanes] for s in range(first, last)], 1)

    def waves(count, start):
        k_lane = lax.broadcasted_iota(jnp.int32, (count, kpad), 1)
        row = lax.broadcasted_iota(jnp.int32, (count, kpad), 0) + start
        ky_row = jnp.where(row < modes // 2, 2 * row, 2 * row - (modes - 1))
        wave_x = k_lane.astype(F32) * unit
        wave_y = ky_row.astype(F32) * unit
        return k_lane, ky_row, wave_x, wave_y, wave_x * wave_x + wave_y * wave_y

    rows_of = lambda re, im: jnp.concatenate([re, im], 0)
    parts_of = lambda first, last: rows_of(
        gathered(slice(0, rows), first, last), gathered(slice(rows, 2 * rows), first, last)
    )
    near = parts_of(0, plan.space // 2)
    far = reversed_lanes(parts_of(plan.space // 2, plan.space))
    for copy in copies[:3]:
        copy.wait()
    cos_sums = product(split(near + far, 3), x_cos(3), NN, FULL)
    sin_sums = product(split(near - far, 3), x_sin(3), NN, FULL)
    sums = (cos_sums[:modes], cos_sums[modes:], sin_sums[:modes], sin_sums[modes:])
    for part in range(4):
        coef_ref[part] = sums[part]
    k_lane, ky_row, wave_x, wave_y, squared = waves(modes, 0)
    live = squared > 0
    inverse_sq = jnp.where(live, 1.0 / jnp.where(live, squared, 1.0), 0.0)
    weight = jnp.where(ky_row == 0, 1.0 / (n * n), 2.0 / (n * n))
    a_re, a_im, b_re, b_im = project(plan, k_lane, *[s * weight for s in sums])
    pa_re, pa_im, pb_re, pb_im = (c * inverse_sq for c in (a_re, a_im, b_re, b_im))
    copies[3].wait()

    def along_quarter(part, lines):
        out = []
        for parity in range(2):
            high, low = split(lines[parity * (modes // 2) : (parity + 1) * (modes // 2)], 2)
            out.append(
                lax.dot_general(
                    inverse_ref[part, parity], jnp.concatenate([high, low, high], 0), NN, preferred_element_type=F32
                )
            )
        return out

    def to_cells(cos_part, sin_part):
        even = product(split(cos_part, 2), x_cos(2), NT, SHORT)
        odd = product(split(sin_part, 2), x_sin(2), NT, SHORT)
        both = jnp.concatenate([even + odd, even - odd], 1)
        cos_a, cos_b = along_quarter(0, both[:modes])
        sin_a, sin_b = along_quarter(1, both[modes:])
        return (cos_a + cos_b, cos_a - cos_b), (sin_b + sin_a, sin_b - sin_a)

    def along_x(cos_re, cos_im, sin_re, sin_im):
        return to_cells(
            rows_of(wave_x * sin_re, wave_x * sin_im), rows_of(-wave_x * cos_re, -wave_x * cos_im)
        )

    def along_y(cos_re, cos_im, sin_re, sin_im):
        return to_cells(
            rows_of(-wave_y * cos_im, wave_y * cos_re), rows_of(-wave_y * sin_im, wave_y * sin_re)
        )

    w_modes, p_modes = (a_re, a_im, b_re, b_im), (pa_re, pa_im, pb_re, pb_im)
    even, odd = [0.0, 0.0], [0.0, 0.0]
    for flow, slope, sign in ((along_y(*p_modes), along_x(*w_modes), 1.0), (along_x(*p_modes), along_y(*w_modes), -1.0)):
        (flow_cos, flow_sin), (slope_cos, slope_sin) = flow, slope
        for at in range(2):
            even[at] = even[at] + sign * (flow_cos[at] * slope_cos[at] + flow_sin[at] * slope_sin[at])
            odd[at] = odd[at] + sign * (flow_cos[at] * slope_sin[at] + flow_sin[at] * slope_cos[at])

    copies[4].wait()
    mirror = jnp.where(own < plan.group // 2, 1.0, -1.0)

    def own_modes(part, folded):
        both = lax.dot_general(
            own_ref[part], jnp.concatenate(split(folded, 2), 0), NN, preferred_element_type=F32
        )
        return both[:block] + both[block:]

    hats = rows_of(own_modes(0, even[0] + mirror * even[1]), own_modes(1, odd[0] - mirror * odd[1]))
    hat_cos = product(split(hats[:, :half] + hats[:, half:], 2), x_cos(2), NN, SHORT)
    hat_sin = product(split(hats[:, :half] - hats[:, half:], 2), x_sin(2), NN, SHORT)
    advect = (hat_cos[:block], hat_cos[block:], hat_sin[:block], hat_sin[block:])

    mine = [coef_ref[part, pl.ds(first, block), :] for part in range(4)]
    k_lane, _, _, _, squared = waves(block, first)
    fade = 1.0 - (DT_STEP * VISCOSITY) * squared
    new = project(plan, k_lane, *[m * fade - DT_STEP * q for m, q in zip(mine, advect)])
    even = product(split(rows_of(new[0], new[1]), 3), x_cos(3), NT, FULL)
    odd = product(split(rows_of(new[2], new[3]), 3), x_sin(3), NT, FULL)
    line = jnp.concatenate([even + odd, reversed_lanes(even - odd)], 1)
    for peer in range(plan.space):
        cut = slice(peer * rows, (peer + 1) * rows)
        out_ref[peer] = jnp.concatenate([line[:block, cut], line[block:, cut]], 1)


def finish_kernel(plan, moved_ref, driving_ref, y0_ref, y1_ref, y2_ref, out_ref):
    rows, modes, n, count = plan.rows, plan.modes, plan.n, plan.count
    ky = lax.broadcasted_iota(jnp.int32, (modes, 2 * rows), 0)
    weight = jnp.where(ky == 0, 1.0 / (n * n), 2.0 / (n * n))
    lines = []
    for member in range(count):
        line = moved_ref[member * plan.group : (member + 1) * plan.group].reshape(modes, 2 * rows)
        lines.append(jnp.transpose(line * weight))
    real = jnp.concatenate([line[:rows] for line in lines], 0)
    imag = jnp.concatenate([line[rows:] for line in lines], 0)
    y_refs = (y0_ref, y1_ref, y2_ref)
    fresh = product(split(real, 3), [ref[:modes] for ref in y_refs], NN, FULL)
    fresh = fresh + product(split(imag, 3), [ref[modes:] for ref in y_refs], NN, FULL)
    forcing = DT_STEP * driving_ref[...]
    for member in range(count):
        out_ref[member] = (fresh[member * rows : (member + 1) * rows] + forcing).astype(BF16)


def probe_kernel(rows, columns, count, offset_ref, mixing_ref, probes_ref, observed_ref, count_ref, total_ref, weight_ref):
    members = mixing_ref.shape[0]
    for m in range(count):
        weights = [mixing_ref[j, offset_ref[0] + m] for j in range(members)]
        share = (1.0 - state_sum_of(weights)) * (1.0 / members)
        for j in range(members):
            weight_ref[pl.ds(m * members + j, 1), :] = jnp.full((1, columns), weights[j] + share, F32)
    probes = probes_ref[...]
    observed = observed_ref[...]
    amount = probes.shape[1]
    row, column = lax.div(probes, columns), lax.rem(probes, columns)
    in_row = lax.broadcasted_iota(jnp.int32, (rows, amount), 0) == row
    in_column = (lax.broadcasted_iota(jnp.int32, (columns, amount), 0) == column).astype(F32).astype(BF16)
    first = observed.astype(BF16)
    rest = observed - first.astype(F32)
    second = rest.astype(BF16)
    third = (rest - second.astype(F32)).astype(BF16)
    left = [in_row.astype(F32)]
    left += [jnp.where(in_row, piece.astype(F32), 0.0) for piece in (first, second, third)]
    left = jnp.concatenate(left, 0).astype(BF16)
    out = lax.dot_general(left, in_column, NT, preferred_element_type=F32)
    count_ref[...] = out[:rows]
    total_ref[...] = out[rows : 2 * rows] + (out[2 * rows : 3 * rows] + out[3 * rows :])


def state_sum_of(values):
    total = values[0]
    for value in values[1:]:
        total = total + value
    return total


def analysis_kernel(values_ref, weight_ref, out_ref):
    members = values_ref.shape[0]
    values = [values_ref[j].astype(F32) for j in range(members)]
    for m in range(out_ref.shape[0]):
        at = m * members
        acc = weight_ref[at : at + 1, :] * values[0]
        for j in range(1, members):
            acc = acc + weight_ref[at + j : at + j + 1, :] * values[j]
        out_ref[m] = acc


def products_kernel(values_ref, number_ref, total_ref, part_ref, row_ref):
    members, rows, columns = values_ref.shape
    values = [values_ref[j].astype(F32) for j in range(members)]
    number = number_ref[...]
    centre = state_sum_of(values) * (1.0 / members)
    surprise = total_ref[...] - number * centre

    def to_row(product):
        line = jnp.sum(product, 0, keepdims=True)
        short = line[:, :LANES]
        for at in range(LANES, columns, LANES):
            short = short + line[:, at : at + LANES]
        return short

    anomaly = [v - centre for v in values]
    for i in range(members):
        weighted = anomaly[i] * number
        for j in range(i + 1):
            row = to_row(weighted * anomaly[j])
            row_ref[j, pl.ds(i, 1), :] = row
            if j != i:
                row_ref[i, pl.ds(j, 1), :] = row
        row_ref[members, pl.ds(i, 1), :] = to_row(anomaly[i] * surprise)
    lane = lax.broadcasted_iota(jnp.int32, (members, LANES), 1)
    tile = jnp.zeros((members, LANES), F32)
    for j in range(members + 1):
        tile = jnp.where(lane == j, jnp.sum(row_ref[j], 1, keepdims=True), tile)
    part_ref[...] = tile


def tree_sum(parts):
    while len(parts) > 1:
        parts = [a + b for a, b in zip(parts[::2], parts[1::2])]
    return parts[0]


def sum_kernel(*refs):
    refs[-1][...] = tree_sum([ref[...] for ref in refs[:-1]])


def total_kernel(probes, *refs):
    spread_ref, projection_ref = refs[-2:]
    total = tree_sum([ref[...] for ref in refs[:-2]])
    members, lanes = total.shape
    spread_ref[...] = total[:, :members] * (1.0 / probes)
    lane = lax.broadcasted_iota(jnp.int32, (members, lanes), 1)
    row = lax.broadcasted_iota(jnp.int32, (members, lanes), 0)
    column = jnp.where(lane == row, total[:, members : members + 1], 0.0)
    projection_ref[...] = jnp.sum(column, 0, keepdims=True)[:, :members] * (1.0 / math.sqrt(probes))


VMEM = pl.BlockSpec(memory_space=pltpu.VMEM)
SMEM = pl.BlockSpec(memory_space=pltpu.SMEM)
HBM = pl.BlockSpec(memory_space=pltpu.HBM)


def local(kernel, name, limit, in_specs, out_shape, scratch=()):
    return pl.pallas_call(
        kernel,
        out_shape=out_shape,
        in_specs=in_specs,
        out_specs=jax.tree.map(lambda _: VMEM, out_shape),
        scratch_shapes=scratch,
        compiler_params=pltpu.CompilerParams(vmem_limit_bytes=limit * MIB),
        name=name,
    )


def on_device(plan, participant_swirls, driving_source, mixing, probes, observed):
    count, rows, n = participant_swirls.shape
    members, space = mixing.shape[0], plan.space
    array = jax.ShapeDtypeStruct
    me = lax.axis_index("space").astype(jnp.int32).reshape(1)
    offset = (lax.axis_index("member") * count).astype(jnp.int32).reshape(1)
    group = plan.group

    def from_peer(value, away):
        return lax.ppermute(value, "space", [(d, d ^ away) for d in range(space)])

    block_shape = (plan.modes, 2 * rows)
    table = pltpu.VMEM((2 * plan.modes, n), BF16)
    sent = local(
        functools.partial(rows_kernel, plan), "rows_to_modes", 8, [SMEM] + [HBM] * 4,
        [array(block_shape, F32)] * count,
        [pltpu.VMEM((count * rows, n), F32), table, table, table,
         pltpu.VMEM((count,) + block_shape, F32), pltpu.SemaphoreType.DMA((4,))],
    )(me, *[pltpu.with_memory_space_constraint(x, pltpu.HBM)
            for x in (participant_swirls.reshape(count * rows, n), *plan.y_table)])
    blocks = []
    for side in range(count):
        base = sent[0] if side == 0 else from_peer(sent[side], side * group)
        blocks += [base] + [from_peer(base, away) for away in range(1, group)]
    number, total, weights = local(
        functools.partial(probe_kernel, rows, n, count), "probe_cells", 16, [SMEM, SMEM, VMEM, VMEM],
        [array((rows, n), F32), array((rows, n), F32), array((count * members, n), F32)],
    )(offset, mixing, probes.reshape(1, -1), observed.reshape(1, -1))
    tables = [*plan.x_table, plan.y_inverse, plan.y_own]
    line = local(
        functools.partial(member_kernel, plan), "member_step", 24, [SMEM] + [HBM] * 5 + [VMEM] * space,
        array((space, plan.block, 2 * rows), F32),
        [pltpu.VMEM((space,) + block_shape, F32)]
        + [pltpu.VMEM(t.shape, BF16) for t in tables[:4]]
        + [pltpu.VMEM(plan.y_own.shape[1:], BF16), pltpu.VMEM((4, plan.modes, plan.kpad), F32)]
        + [pltpu.SemaphoreType.DMA((5,))],
    )(me, *[pltpu.with_memory_space_constraint(t, pltpu.HBM) for t in tables], *blocks)
    moved = lax.all_to_all(line, "space", split_axis=0, concat_axis=0, tiled=True)
    rounded = local(
        functools.partial(finish_kernel, plan), "modes_to_rows", 8, [VMEM] * 5, array((count, rows, n), BF16)
    )(moved, driving_source, *plan.y_table)
    values = lax.all_gather(rounded, "member", axis=0, tiled=True)
    tile = array((members, LANES), F32)
    part = local(
        products_kernel, "products", 16, [VMEM] * 3, tile, [pltpu.VMEM((members + 1, members, LANES), F32)]
    )(values, number, total)
    part = local(sum_kernel, "side_sum", 4, [VMEM] * group, tile)(
        part, *[from_peer(part, away) for away in range(1, group)]
    )
    analysis = local(
        analysis_kernel, "analysis", 16, [VMEM] * 2, array((count, rows, n), F32)
    )(values, weights)
    spread, projection = local(
        functools.partial(total_kernel, probes.shape[0] * space), "probe_totals", 4, [VMEM] * count,
        [array((members, members), F32), array((1, members), F32)],
    )(part, *[from_peer(part, side * group) for side in range(1, count)])
    return analysis, spread, projection.reshape(members)


def solution(mesh):
    space = mesh.shape["space"]

    def body(participant_swirls, *rest):
        count, rows, n = participant_swirls.shape
        return on_device(Plan(n, rows, space, count), participant_swirls, *rest)

    return jax.shard_map(
        body,
        mesh=mesh,
        in_specs=(P("member", "space", None), P("space", None), P(), P("space"), P("space")),
        out_specs=(P("member", "space", None), P(), P()),
        check_vma=False,
    )
```

```python
import functools
import math

import jax
import jax.numpy as jnp
import numpy as np
from jax import lax
from jax.experimental import pallas as pl
from jax.experimental.pallas import tpu as pltpu
from jax.sharding import PartitionSpec as P

KEEP = 160
DT_STEP = 0.1
VISCOSITY = 0.05
LANES = 128
F32 = jnp.float32
BF16 = jnp.bfloat16

NN = (((1,), (0,)), ((), ()))
NT = (((1,), (1,)), ((), ()))
FULL = ((0, 0), (0, 1), (1, 0), (1, 1), (0, 2), (2, 0))
SHORT = ((0, 0), (0, 1), (1, 0))
MIB = 1 << 20


def round_up(value, unit):
    return -(-value // unit) * unit


def split_table(table, pieces):
    rest, out = np.asarray(table, np.float64), []
    for _ in range(pieces):
        out.append(rest.astype(np.float32).astype(BF16))
        rest = rest - out[-1].astype(np.float64)
    return tuple(jnp.asarray(piece) for piece in out)


def split(value, pieces):
    out = []
    for piece in range(pieces):
        out.append(value.astype(BF16))
        if piece + 1 < pieces:
            value = value - out[-1].astype(F32)
    return out


def product(left, right, dims, terms):
    out = None
    for i, j in reversed(terms):
        term = lax.dot_general(left[i], right[j], dims, preferred_element_type=F32)
        out = term if out is None else out + term
    return out


class Plan:
    def __init__(self, n, rows, space, count):
        self.n, self.rows, self.space, self.count = n, rows, space, count
        self.group = space // count
        self.block = round_up(-(-KEEP // self.group), 8)
        self.modes = self.block * self.group
        self.half = n // 2
        self.kpad = round_up(KEEP + 1, LANES)
        cells = np.arange(n) + 0.5
        scale = 2.0 * math.pi / n
        ky = np.concatenate([np.arange(0, self.modes, 2), np.arange(1, self.modes, 2)])
        live = (ky < KEEP)[:, None]
        angle_y = scale * ky[:, None] * cells[None, :]
        waves_y = np.stack([np.cos(angle_y) * live, -np.sin(angle_y) * live])
        self.y_table = split_table(waves_y[:, :, : self.half].reshape(2 * self.modes, self.half), 3)
        quarter = waves_y[:, :, : n // 4]
        self.quarter = n // 4
        high, low = split_table(quarter.reshape(2, 2, self.modes // 2, n // 4).transpose(0, 1, 3, 2), 2)
        self.y_inverse = jnp.concatenate([high, high, low], -1)
        own = 2.0 * quarter.reshape(2, self.group, self.block, n // 4).transpose(1, 0, 2, 3)
        high, low = split_table(own, 2)
        self.y_own = jnp.concatenate(
            [jnp.concatenate([high, high], -1), jnp.concatenate([low, jnp.zeros_like(low)], -1)], -2
        )
        kx = np.arange(self.kpad)
        angle_x = scale * cells[: self.half, None] * kx[None, :]
        keep_x = (kx <= KEEP)[None, :]
        self.x_table = split_table(np.concatenate([np.cos(angle_x) * keep_x, np.sin(angle_x) * keep_x], 1), 3)


def reversed_lanes(value):
    width = value.shape[1]
    swap = lax.broadcasted_iota(jnp.int32, (width, width), 0) + lax.broadcasted_iota(jnp.int32, (width, width), 1)
    swap = jnp.where(swap == width - 1, 1.0, 0.0).astype(BF16)
    return product(split(value, 3), [swap], NN, ((0, 0), (1, 0), (2, 0)))


def rows_kernel(plan, me_ref, field_hbm, y0_hbm, y1_hbm, y2_hbm, x0_hbm, x1_hbm, x2_hbm, *refs):
    rows, modes, count, half = plan.rows, plan.modes, plan.count, plan.half
    outs, x_outs = refs[:count], refs[count : count + 3]
    field_ref, y0_ref, y1_ref, y2_ref, packed_ref, sems = refs[count + 3 :]
    sources = (field_hbm, y0_hbm, y1_hbm, y2_hbm, x0_hbm, x1_hbm, x2_hbm)
    targets = (field_ref, y0_ref, y1_ref, y2_ref, *x_outs)
    copies = [pltpu.make_async_copy(s, t, sems.at[i]) for i, (s, t) in enumerate(zip(sources, targets))]
    for copy in copies:
        copy.start()
    copies[0].wait()
    far = reversed_lanes(field_ref[:, half:])
    even, odd = split(field_ref[:, :half] + far, 3), split(field_ref[:, :half] - far, 3)
    for copy in copies[1:4]:
        copy.wait()
    y_refs = (y0_ref, y1_ref, y2_ref)
    real = product([ref[:modes] for ref in y_refs], even, NT, FULL)
    imag = product([ref[modes:] for ref in y_refs], odd, NT, FULL)
    for member in range(count):
        at = slice(member * rows, (member + 1) * rows)
        packed_ref[member] = jnp.concatenate([real[:, at], imag[:, at]], 1)
    side = me_ref[0] // plan.group
    for away in range(count):
        outs[away][...] = packed_ref[side ^ away]
    for copy in copies[4:]:
        copy.wait()


def project(plan, k_lane, cos_re, cos_im, sin_re, sin_im):
    weight = jnp.where((k_lane == 0) | (k_lane == KEEP), 1.0, 2.0)
    edge = jnp.where(k_lane == KEEP, 1.0, 0.0)
    return (
        weight * cos_re - edge * sin_im,
        weight * cos_im + edge * sin_re,
        weight * sin_re + edge * cos_im,
        weight * sin_im - edge * cos_re,
    )


def member_kernel(plan, me_ref, inverse_hbm, own_hbm, x0_ref, x1_ref, x2_ref, *refs):
    blocks, out_ref, moved_ref = refs[: plan.space], refs[plan.space], refs[plan.space + 1]
    inverse_ref, own_ref, coef_ref, sems = refs[plan.space + 2 :]
    me = me_ref[0]
    own = me % plan.group
    copies = [
        pltpu.make_async_copy(inverse_hbm, inverse_ref, sems.at[0]),
        pltpu.make_async_copy(own_hbm.at[own], own_ref, sems.at[1]),
    ]
    for copy in copies:
        copy.start()
    for away in range(plan.space):
        moved_ref[me ^ away] = blocks[away][...]
    n, half, modes, block, kpad, rows = plan.n, plan.half, plan.modes, plan.block, plan.kpad, plan.rows
    unit = 2.0 * math.pi / n
    first = pl.multiple_of(own * block, 8)
    x_refs = (x0_ref, x1_ref, x2_ref)

    def x_cos(pieces):
        return [ref[:, :kpad] for ref in x_refs[:pieces]]

    def x_sin(pieces):
        return [ref[:, kpad:] for ref in x_refs[:pieces]]

    def gathered(lanes, first, last):
        return jnp.concatenate([moved_ref[s, :, lanes] for s in range(first, last)], 1)

    def waves(count, start):
        k_lane = lax.broadcasted_iota(jnp.int32, (count, kpad), 1)
        row = lax.broadcasted_iota(jnp.int32, (count, kpad), 0) + start
        ky_row = jnp.where(row < modes // 2, 2 * row, 2 * row - (modes - 1))
        wave_x = k_lane.astype(F32) * unit
        wave_y = ky_row.astype(F32) * unit
        return k_lane, ky_row, wave_x, wave_y, wave_x * wave_x + wave_y * wave_y

    rows_of = lambda re, im: jnp.concatenate([re, im], 0)
    parts_of = lambda first, last: rows_of(
        gathered(slice(0, rows), first, last), gathered(slice(rows, 2 * rows), first, last)
    )
    near = parts_of(0, plan.space // 2)
    far = reversed_lanes(parts_of(plan.space // 2, plan.space))
    cos_sums = product(split(near + far, 3), x_cos(3), NN, FULL)
    sin_sums = product(split(near - far, 3), x_sin(3), NN, FULL)
    sums = (cos_sums[:modes], cos_sums[modes:], sin_sums[:modes], sin_sums[modes:])
    for part in range(4):
        coef_ref[part] = sums[part]
    k_lane, ky_row, wave_x, wave_y, squared = waves(modes, 0)
    live = squared > 0
    inverse_sq = jnp.where(live, 1.0 / jnp.where(live, squared, 1.0), 0.0)
    weight = jnp.where(ky_row == 0, 1.0 / (n * n), 2.0 / (n * n))
    a_re, a_im, b_re, b_im = project(plan, k_lane, *[s * weight for s in sums])
    pa_re, pa_im, pb_re, pb_im = (c * inverse_sq for c in (a_re, a_im, b_re, b_im))
    copies[0].wait()

    def along_quarter(part, lines):
        out = []
        for parity in range(2):
            high, low = split(lines[parity * (modes // 2) : (parity + 1) * (modes // 2)], 2)
            out.append(
                lax.dot_general(
                    inverse_ref[part, parity], jnp.concatenate([high, low, high], 0), NN, preferred_element_type=F32
                )
            )
        return out

    def to_cells(cos_part, sin_part):
        even = product(split(cos_part, 2), x_cos(2), NT, SHORT)
        odd = product(split(sin_part, 2), x_sin(2), NT, SHORT)
        both = jnp.concatenate([even + odd, even - odd], 1)
        cos_a, cos_b = along_quarter(0, both[:modes])
        sin_a, sin_b = along_quarter(1, both[modes:])
        return (cos_a + cos_b, cos_a - cos_b), (sin_b + sin_a, sin_b - sin_a)

    def along_x(cos_re, cos_im, sin_re, sin_im):
        return to_cells(
            rows_of(wave_x * sin_re, wave_x * sin_im), rows_of(-wave_x * cos_re, -wave_x * cos_im)
        )

    def along_y(cos_re, cos_im, sin_re, sin_im):
        return to_cells(
            rows_of(-wave_y * cos_im, wave_y * cos_re), rows_of(-wave_y * sin_im, wave_y * sin_re)
        )

    w_modes, p_modes = (a_re, a_im, b_re, b_im), (pa_re, pa_im, pb_re, pb_im)
    even, odd = [0.0, 0.0], [0.0, 0.0]
    for flow, slope, sign in ((along_y(*p_modes), along_x(*w_modes), 1.0), (along_x(*p_modes), along_y(*w_modes), -1.0)):
        (flow_cos, flow_sin), (slope_cos, slope_sin) = flow, slope
        for at in range(2):
            even[at] = even[at] + sign * (flow_cos[at] * slope_cos[at] + flow_sin[at] * slope_sin[at])
            odd[at] = odd[at] + sign * (flow_cos[at] * slope_sin[at] + flow_sin[at] * slope_cos[at])

    copies[1].wait()
    mirror = jnp.where(own < plan.group // 2, 1.0, -1.0)

    def own_modes(part, folded):
        both = lax.dot_general(
            own_ref[part], jnp.concatenate(split(folded, 2), 0), NN, preferred_element_type=F32
        )
        return both[:block] + both[block:]

    hats = rows_of(own_modes(0, even[0] + mirror * even[1]), own_modes(1, odd[0] - mirror * odd[1]))
    hat_cos = product(split(hats[:, :half] + hats[:, half:], 2), x_cos(2), NN, SHORT)
    hat_sin = product(split(hats[:, :half] - hats[:, half:], 2), x_sin(2), NN, SHORT)
    advect = (hat_cos[:block], hat_cos[block:], hat_sin[:block], hat_sin[block:])

    mine = [coef_ref[part, pl.ds(first, block), :] for part in range(4)]
    k_lane, _, _, _, squared = waves(block, first)
    fade = 1.0 - (DT_STEP * VISCOSITY) * squared
    new = project(plan, k_lane, *[m * fade - DT_STEP * q for m, q in zip(mine, advect)])
    even = product(split(rows_of(new[0], new[1]), 3), x_cos(3), NT, FULL)
    odd = product(split(rows_of(new[2], new[3]), 3), x_sin(3), NT, FULL)
    line = jnp.concatenate([even + odd, reversed_lanes(even - odd)], 1)
    for peer in range(plan.space):
        cut = slice(peer * rows, (peer + 1) * rows)
        out_ref[peer] = jnp.concatenate([line[:block, cut], line[block:, cut]], 1)


def finish_kernel(plan, moved_ref, driving_ref, y0_ref, y1_ref, y2_ref, out_ref):
    rows, modes, n, count = plan.rows, plan.modes, plan.n, plan.count
    ky = lax.broadcasted_iota(jnp.int32, (modes, 2 * rows), 0)
    weight = jnp.where(ky == 0, 1.0 / (n * n), 2.0 / (n * n))
    lines = []
    for member in range(count):
        line = moved_ref[member * plan.group : (member + 1) * plan.group].reshape(modes, 2 * rows)
        lines.append(jnp.transpose(line * weight))
    real = jnp.concatenate([line[:rows] for line in lines], 0)
    imag = jnp.concatenate([line[rows:] for line in lines], 0)
    y_refs = (y0_ref, y1_ref, y2_ref)
    even = product(split(real, 3), [ref[:modes] for ref in y_refs], NN, FULL)
    odd = product(split(imag, 3), [ref[modes:] for ref in y_refs], NN, FULL)
    fresh = jnp.concatenate([even + odd, reversed_lanes(even - odd)], 1)
    forcing = DT_STEP * driving_ref[...]
    for member in range(count):
        out_ref[member] = (fresh[member * rows : (member + 1) * rows] + forcing).astype(BF16)


def probe_kernel(rows, columns, count, offset_ref, mixing_ref, probes_ref, observed_ref, count_ref, total_ref, weight_ref):
    members = mixing_ref.shape[0]
    for m in range(count):
        weights = [mixing_ref[j, offset_ref[0] + m] for j in range(members)]
        share = (1.0 - state_sum_of(weights)) * (1.0 / members)
        for j in range(members):
            weight_ref[pl.ds(m * members + j, 1), :] = jnp.full((1, columns), weights[j] + share, F32)
    probes = probes_ref[...]
    observed = observed_ref[...]
    amount = probes.shape[1]
    row, column = lax.div(probes, columns), lax.rem(probes, columns)
    in_row = lax.broadcasted_iota(jnp.int32, (rows, amount), 0) == row
    in_column = (lax.broadcasted_iota(jnp.int32, (columns, amount), 0) == column).astype(F32).astype(BF16)
    first = observed.astype(BF16)
    rest = observed - first.astype(F32)
    second = rest.astype(BF16)
    third = (rest - second.astype(F32)).astype(BF16)
    left = [in_row.astype(F32)]
    left += [jnp.where(in_row, piece.astype(F32), 0.0) for piece in (first, second, third)]
    left = jnp.concatenate(left, 0).astype(BF16)
    out = lax.dot_general(left, in_column, NT, preferred_element_type=F32)
    count_ref[...] = out[:rows]
    total_ref[...] = out[rows : 2 * rows] + (out[2 * rows : 3 * rows] + out[3 * rows :])


def state_sum_of(values):
    total = values[0]
    for value in values[1:]:
        total = total + value
    return total


def analysis_kernel(values_ref, weight_ref, out_ref):
    members = values_ref.shape[0]
    values = [values_ref[j].astype(F32) for j in range(members)]
    for m in range(out_ref.shape[0]):
        at = m * members
        acc = weight_ref[at : at + 1, :] * values[0]
        for j in range(1, members):
            acc = acc + weight_ref[at + j : at + j + 1, :] * values[j]
        out_ref[m] = acc


def products_kernel(values_ref, number_ref, total_ref, part_ref, row_ref):
    members, rows, columns = values_ref.shape
    values = [values_ref[j].astype(F32) for j in range(members)]
    number = number_ref[...]
    centre = state_sum_of(values) * (1.0 / members)
    surprise = total_ref[...] - number * centre

    def to_row(product):
        line = jnp.sum(product, 0, keepdims=True)
        short = line[:, :LANES]
        for at in range(LANES, columns, LANES):
            short = short + line[:, at : at + LANES]
        return short

    anomaly = [v - centre for v in values]
    for i in range(members):
        weighted = anomaly[i] * number
        for j in range(i + 1):
            row = to_row(weighted * anomaly[j])
            row_ref[j, pl.ds(i, 1), :] = row
            if j != i:
                row_ref[i, pl.ds(j, 1), :] = row
        row_ref[members, pl.ds(i, 1), :] = to_row(anomaly[i] * surprise)
    lane = lax.broadcasted_iota(jnp.int32, (members, LANES), 1)
    tile = jnp.zeros((members, LANES), F32)
    for j in range(members + 1):
        tile = jnp.where(lane == j, jnp.sum(row_ref[j], 1, keepdims=True), tile)
    for peer in range(part_ref.shape[0]):
        part_ref[peer] = tile


def total_kernel(probes, parts_ref, spread_ref, projection_ref):
    copies, members, lanes = parts_ref.shape
    total = parts_ref[0]
    for s in range(1, copies):
        total = total + parts_ref[s]
    spread_ref[...] = total[:, :members] * (1.0 / probes)
    lane = lax.broadcasted_iota(jnp.int32, (members, lanes), 1)
    row = lax.broadcasted_iota(jnp.int32, (members, lanes), 0)
    column = jnp.where(lane == row, total[:, members : members + 1], 0.0)
    projection_ref[...] = jnp.sum(column, 0, keepdims=True)[:, :members] * (1.0 / math.sqrt(probes))


VMEM = pl.BlockSpec(memory_space=pltpu.VMEM)
SMEM = pl.BlockSpec(memory_space=pltpu.SMEM)
HBM = pl.BlockSpec(memory_space=pltpu.HBM)


def local(kernel, name, limit, in_specs, out_shape, scratch=()):
    return pl.pallas_call(
        kernel,
        out_shape=out_shape,
        in_specs=in_specs,
        out_specs=jax.tree.map(lambda _: VMEM, out_shape),
        scratch_shapes=scratch,
        compiler_params=pltpu.CompilerParams(vmem_limit_bytes=limit * MIB),
        name=name,
    )


def on_device(plan, participant_swirls, driving_source, mixing, probes, observed):
    count, rows, n = participant_swirls.shape
    members, space = mixing.shape[0], plan.space
    array = jax.ShapeDtypeStruct
    me = lax.axis_index("space").astype(jnp.int32).reshape(1)
    offset = (lax.axis_index("member") * count).astype(jnp.int32).reshape(1)
    group = plan.group
    exchange = functools.partial(lax.all_to_all, axis_name="space", split_axis=0, concat_axis=0, tiled=True)

    def from_peer(value, away):
        return lax.ppermute(value, "space", [(d, d ^ away) for d in range(space)])

    block_shape = (plan.modes, 2 * rows)
    table = pltpu.VMEM(plan.y_table[0].shape, BF16)
    sent = local(
        functools.partial(rows_kernel, plan), "rows_to_modes", 8, [SMEM] + [HBM] * 7,
        [array(block_shape, F32)] * count + [array(t.shape, BF16) for t in plan.x_table],
        [pltpu.VMEM((count * rows, n), F32), table, table, table,
         pltpu.VMEM((count,) + block_shape, F32), pltpu.SemaphoreType.DMA((7,))],
    )(me, *[pltpu.with_memory_space_constraint(x, pltpu.HBM)
            for x in (participant_swirls.reshape(count * rows, n), *plan.y_table, *plan.x_table)])
    sent, x_table = sent[:count], sent[count:]
    blocks = []
    for side in range(count):
        base = sent[0] if side == 0 else from_peer(sent[side], side * group)
        blocks += [base] + [from_peer(base, away) for away in range(1, group)]
    number, total, weights = local(
        functools.partial(probe_kernel, rows, n, count), "probe_cells", 16, [SMEM, SMEM, VMEM, VMEM],
        [array((rows, n), F32), array((rows, n), F32), array((count * members, n), F32)],
    )(offset, mixing, probes.reshape(1, -1), observed.reshape(1, -1))
    tables = [plan.y_inverse, plan.y_own]
    line = local(
        functools.partial(member_kernel, plan), "member_step", 24, [SMEM] + [HBM] * 2 + [VMEM] * (3 + space),
        array((space, plan.block, 2 * rows), F32),
        [pltpu.VMEM((space,) + block_shape, F32), pltpu.VMEM(plan.y_inverse.shape, BF16),
         pltpu.VMEM(plan.y_own.shape[1:], BF16), pltpu.VMEM((4, plan.modes, plan.kpad), F32),
         pltpu.SemaphoreType.DMA((2,))],
    )(me, *[pltpu.with_memory_space_constraint(t, pltpu.HBM) for t in tables], *x_table, *blocks)
    moved = exchange(line)
    rounded = local(
        functools.partial(finish_kernel, plan), "modes_to_rows", 8, [VMEM] * 5, array((count, rows, n), BF16)
    )(moved, driving_source, *plan.y_table)
    values = lax.all_gather(rounded, "member", axis=0, tiled=True)
    part = local(
        products_kernel, "products", 16, [VMEM] * 3, array((space, members, LANES), F32),
        [pltpu.VMEM((members + 1, members, LANES), F32)],
    )(values, number, total)
    parts = exchange(part)
    analysis = local(
        analysis_kernel, "analysis", 16, [VMEM] * 2, array((count, rows, n), F32)
    )(values, weights)
    spread, projection = local(
        functools.partial(total_kernel, probes.shape[0] * space), "probe_totals", 4, [VMEM],
        [array((members, members), F32), array((1, members), F32)],
    )(parts)
    return analysis, spread, projection.reshape(members)


def solution(mesh):
    space = mesh.shape["space"]

    def body(participant_swirls, *rest):
        count, rows, n = participant_swirls.shape
        return on_device(Plan(n, rows, space, count), participant_swirls, *rest)

    return jax.shard_map(
        body,
        mesh=mesh,
        in_specs=(P("member", "space", None), P("space", None), P(), P("space"), P("space")),
        out_specs=(P("member", "space", None), P(), P()),
        check_vma=False,
    )
```

```python
import functools
import math

import jax
import jax.numpy as jnp
import numpy as np
from jax import lax
from jax.experimental import pallas as pl
from jax.experimental.pallas import tpu as pltpu
from jax.sharding import PartitionSpec as P

KEEP = 160
DT_STEP = 0.1
VISCOSITY = 0.05
LANES = 128
F32 = jnp.float32
BF16 = jnp.bfloat16

NN = (((1,), (0,)), ((), ()))
NT = (((1,), (1,)), ((), ()))
FULL = ((0, 0), (0, 1), (1, 0), (1, 1), (0, 2), (2, 0))
SHORT = ((0, 0), (0, 1), (1, 0))
MIB = 1 << 20


def round_up(value, unit):
    return -(-value // unit) * unit


def split_table(table, pieces):
    rest, out = np.asarray(table, np.float64), []
    for _ in range(pieces):
        out.append(rest.astype(np.float32).astype(BF16))
        rest = rest - out[-1].astype(np.float64)
    return tuple(jnp.asarray(piece) for piece in out)


def split(value, pieces):
    out = []
    for piece in range(pieces):
        out.append(value.astype(BF16))
        if piece + 1 < pieces:
            value = value - out[-1].astype(F32)
    return out


def product(left, right, dims, terms):
    out = None
    for i, j in reversed(terms):
        term = lax.dot_general(left[i], right[j], dims, preferred_element_type=F32)
        out = term if out is None else out + term
    return out


class Plan:
    def __init__(self, n, rows, space, count):
        self.n, self.rows, self.space, self.count = n, rows, space, count
        self.group = space // count
        self.block = round_up(-(-KEEP // self.group), 8)
        self.modes = self.block * self.group
        self.half = n // 2
        self.kpad = round_up(KEEP + 1, LANES)
        cells = np.arange(n) + 0.5
        scale = 2.0 * math.pi / n
        ky = np.concatenate([np.arange(0, self.modes, 2), np.arange(1, self.modes, 2)])
        live = (ky < KEEP)[:, None]
        angle_y = scale * ky[:, None] * cells[None, :]
        waves_y = np.stack([np.cos(angle_y) * live, -np.sin(angle_y) * live])
        self.y_table = split_table(waves_y[:, :, : self.half].reshape(2 * self.modes, self.half), 3)
        quarter = waves_y[:, :, : n // 4]
        self.quarter = n // 4
        high, low = split_table(quarter.reshape(2, 2, self.modes // 2, n // 4).transpose(0, 1, 3, 2), 2)
        self.y_inverse = jnp.concatenate([high, high, low], -1)
        own = 2.0 * quarter.reshape(2, self.group, self.block, n // 4).transpose(1, 0, 2, 3)
        high, low = split_table(own, 2)
        self.y_own = jnp.concatenate(
            [jnp.concatenate([high, high], -1), jnp.concatenate([low, jnp.zeros_like(low)], -1)], -2
        )
        kx = np.arange(self.kpad)
        angle_x = scale * cells[: self.half, None] * kx[None, :]
        keep_x = (kx <= KEEP)[None, :]
        self.x_table = split_table(np.concatenate([np.cos(angle_x) * keep_x, np.sin(angle_x) * keep_x], 1), 3)
        self.main = self.kpad - LANES
        self.step = round_up(KEEP + 1 - self.main, 8)
        high, low = (table.reshape(self.half, 2, self.kpad).transpose(1, 2, 0) for table in self.x_table[:2])
        tails = [table[:, self.main : self.main + self.step] for table in (high, high, low)]
        empty = jnp.zeros((2, LANES - 3 * self.step, self.half), BF16)
        self.x_inverse = jnp.concatenate([t[:, : self.main] for t in (high, high, low)] + tails + [empty], 1)


def reversed_lanes(value):
    width = value.shape[1]
    swap = lax.broadcasted_iota(jnp.int32, (width, width), 0) + lax.broadcasted_iota(jnp.int32, (width, width), 1)
    swap = jnp.where(swap == width - 1, 1.0, 0.0).astype(BF16)
    return product(split(value, 3), [swap], NN, ((0, 0), (1, 0), (2, 0)))


def start_copies(sources, targets, sems):
    copies = [pltpu.make_async_copy(s, t, sems.at[i]) for i, (s, t) in enumerate(zip(sources, targets))]
    for copy in copies:
        copy.start()
    return copies


def rows_kernel(plan, me_ref, field_hbm, y0_hbm, y1_hbm, y2_hbm, *refs):
    rows, modes, count, half = plan.rows, plan.modes, plan.count, plan.half
    outs, (field_ref, y0_ref, y1_ref, y2_ref, packed_ref, sems) = refs[:count], refs[count:]
    copies = start_copies((field_hbm, y0_hbm, y1_hbm, y2_hbm), (field_ref, y0_ref, y1_ref, y2_ref), sems)
    copies[0].wait()
    far = reversed_lanes(field_ref[:, half:])
    even, odd = split(field_ref[:, :half] + far, 3), split(field_ref[:, :half] - far, 3)
    for copy in copies[1:]:
        copy.wait()
    y_refs = (y0_ref, y1_ref, y2_ref)
    real = product([ref[:modes] for ref in y_refs], even, NT, FULL)
    imag = product([ref[modes:] for ref in y_refs], odd, NT, FULL)
    for member in range(count):
        at = slice(member * rows, (member + 1) * rows)
        packed_ref[member] = jnp.concatenate([real[:, at], imag[:, at]], 1)
    side = me_ref[0] // plan.group
    for away in range(count):
        outs[away][...] = packed_ref[side ^ away]


def project(plan, k_lane, cos_re, cos_im, sin_re, sin_im):
    weight = jnp.where((k_lane == 0) | (k_lane == KEEP), 1.0, 2.0)
    edge = jnp.where(k_lane == KEEP, 1.0, 0.0)
    return (
        weight * cos_re - edge * sin_im,
        weight * cos_im + edge * sin_re,
        weight * sin_re + edge * cos_im,
        weight * sin_im - edge * cos_re,
    )


def pack_lines(plan, value):
    high, low = split(value, 2)
    main = [piece[:, : plan.main] for piece in (high, low, high)]
    last_high, last_low = (piece[:, plan.main :].astype(F32) for piece in (high, low))
    tail = last_high + pltpu.roll(last_low, plan.step, 1) + pltpu.roll(last_high, 2 * plan.step, 1)
    return jnp.concatenate(main + [tail.astype(BF16)], 1)


def member_kernel(plan, me_ref, inverse_hbm, own_hbm, lines_hbm, x0_ref, x1_ref, x2_ref, *refs):
    blocks, out_ref, moved_ref = refs[: plan.space], refs[plan.space], refs[plan.space + 1]
    inverse_ref, own_ref, lines_ref, coef_ref, sems = refs[plan.space + 2 :]
    me = me_ref[0]
    own = me % plan.group
    copies = start_copies((inverse_hbm, own_hbm.at[own], lines_hbm), (inverse_ref, own_ref, lines_ref), sems)
    for away in range(plan.space):
        moved_ref[me ^ away] = blocks[away][...]
    n, half, modes, block, kpad, rows = plan.n, plan.half, plan.modes, plan.block, plan.kpad, plan.rows
    unit = 2.0 * math.pi / n
    first = pl.multiple_of(own * block, 8)
    x_refs = (x0_ref, x1_ref, x2_ref)

    def x_cos(pieces):
        return [ref[:, :kpad] for ref in x_refs[:pieces]]

    def x_sin(pieces):
        return [ref[:, kpad:] for ref in x_refs[:pieces]]

    def gathered(lanes, first, last):
        return jnp.concatenate([moved_ref[s, :, lanes] for s in range(first, last)], 1)

    def waves(count, start):
        k_lane = lax.broadcasted_iota(jnp.int32, (count, kpad), 1)
        row = lax.broadcasted_iota(jnp.int32, (count, kpad), 0) + start
        ky_row = jnp.where(row < modes // 2, 2 * row, 2 * row - (modes - 1))
        wave_x = k_lane.astype(F32) * unit
        wave_y = ky_row.astype(F32) * unit
        return k_lane, ky_row, wave_x, wave_y, wave_x * wave_x + wave_y * wave_y

    rows_of = lambda re, im: jnp.concatenate([re, im], 0)
    parts_of = lambda first, last: rows_of(
        gathered(slice(0, rows), first, last), gathered(slice(rows, 2 * rows), first, last)
    )
    near = parts_of(0, plan.space // 2)
    far = reversed_lanes(parts_of(plan.space // 2, plan.space))
    cos_sums = product(split(near + far, 3), x_cos(3), NN, FULL)
    sin_sums = product(split(near - far, 3), x_sin(3), NN, FULL)
    sums = (cos_sums[:modes], cos_sums[modes:], sin_sums[:modes], sin_sums[modes:])
    for part in range(4):
        coef_ref[part] = sums[part]
    k_lane, ky_row, wave_x, wave_y, squared = waves(modes, 0)
    live = squared > 0
    inverse_sq = jnp.where(live, 1.0 / jnp.where(live, squared, 1.0), 0.0)
    weight = jnp.where(ky_row == 0, 1.0 / (n * n), 2.0 / (n * n))
    a_re, a_im, b_re, b_im = project(plan, k_lane, *[s * weight for s in sums])
    pa_re, pa_im, pb_re, pb_im = (c * inverse_sq for c in (a_re, a_im, b_re, b_im))
    copies[0].wait()
    copies[2].wait()

    def along_quarter(part, lines):
        out = []
        for parity in range(2):
            high, low = split(lines[parity * (modes // 2) : (parity + 1) * (modes // 2)], 2)
            out.append(
                lax.dot_general(
                    inverse_ref[part, parity], jnp.concatenate([high, low, high], 0), NN, preferred_element_type=F32
                )
            )
        return out

    def to_cells(cos_part, sin_part):
        even = lax.dot_general(pack_lines(plan, cos_part), lines_ref[0], NN, preferred_element_type=F32)
        odd = lax.dot_general(pack_lines(plan, sin_part), lines_ref[1], NN, preferred_element_type=F32)
        both = jnp.concatenate([even + odd, even - odd], 1)
        cos_a, cos_b = along_quarter(0, both[:modes])
        sin_a, sin_b = along_quarter(1, both[modes:])
        return (cos_a + cos_b, cos_a - cos_b), (sin_b + sin_a, sin_b - sin_a)

    def along_x(cos_re, cos_im, sin_re, sin_im):
        return to_cells(
            rows_of(wave_x * sin_re, wave_x * sin_im), rows_of(-wave_x * cos_re, -wave_x * cos_im)
        )

    def along_y(cos_re, cos_im, sin_re, sin_im):
        return to_cells(
            rows_of(-wave_y * cos_im, wave_y * cos_re), rows_of(-wave_y * sin_im, wave_y * sin_re)
        )

    w_modes, p_modes = (a_re, a_im, b_re, b_im), (pa_re, pa_im, pb_re, pb_im)
    even, odd = [0.0, 0.0], [0.0, 0.0]
    for flow, slope, sign in ((along_y(*p_modes), along_x(*w_modes), 1.0), (along_x(*p_modes), along_y(*w_modes), -1.0)):
        (flow_cos, flow_sin), (slope_cos, slope_sin) = flow, slope
        for at in range(2):
            even[at] = even[at] + sign * (flow_cos[at] * slope_cos[at] + flow_sin[at] * slope_sin[at])
            odd[at] = odd[at] + sign * (flow_cos[at] * slope_sin[at] + flow_sin[at] * slope_cos[at])

    copies[1].wait()
    mirror = jnp.where(own < plan.group // 2, 1.0, -1.0)

    def own_modes(part, folded):
        both = lax.dot_general(
            own_ref[part], jnp.concatenate(split(folded, 2), 0), NN, preferred_element_type=F32
        )
        return both[:block] + both[block:]

    hats = rows_of(own_modes(0, even[0] + mirror * even[1]), own_modes(1, odd[0] - mirror * odd[1]))
    hat_cos = product(split(hats[:, :half] + hats[:, half:], 2), x_cos(2), NN, SHORT)
    hat_sin = product(split(hats[:, :half] - hats[:, half:], 2), x_sin(2), NN, SHORT)
    advect = (hat_cos[:block], hat_cos[block:], hat_sin[:block], hat_sin[block:])

    mine = [coef_ref[part, pl.ds(first, block), :] for part in range(4)]
    k_lane, _, _, _, squared = waves(block, first)
    fade = 1.0 - (DT_STEP * VISCOSITY) * squared
    new = project(plan, k_lane, *[m * fade - DT_STEP * q for m, q in zip(mine, advect)])
    even = product(split(rows_of(new[0], new[1]), 3), x_cos(3), NT, FULL)
    odd = product(split(rows_of(new[2], new[3]), 3), x_sin(3), NT, FULL)
    line = jnp.concatenate([even + odd, reversed_lanes(even - odd)], 1)
    for peer in range(plan.space):
        cut = slice(peer * rows, (peer + 1) * rows)
        out_ref[peer] = jnp.concatenate([line[:block, cut], line[block:, cut]], 1)


def finish_kernel(plan, moved_ref, driving_ref, y0_ref, y1_ref, y2_ref, out_ref):
    rows, modes, n, count = plan.rows, plan.modes, plan.n, plan.count
    ky = lax.broadcasted_iota(jnp.int32, (modes, 2 * rows), 0)
    weight = jnp.where(ky == 0, 1.0 / (n * n), 2.0 / (n * n))
    lines = []
    for member in range(count):
        line = moved_ref[member * plan.group : (member + 1) * plan.group].reshape(modes, 2 * rows)
        lines.append(jnp.transpose(line * weight))
    real = jnp.concatenate([line[:rows] for line in lines], 0)
    imag = jnp.concatenate([line[rows:] for line in lines], 0)
    y_refs = (y0_ref, y1_ref, y2_ref)
    even = product(split(real, 3), [ref[:modes] for ref in y_refs], NN, FULL)
    odd = product(split(imag, 3), [ref[modes:] for ref in y_refs], NN, FULL)
    fresh = jnp.concatenate([even + odd, reversed_lanes(even - odd)], 1)
    forcing = DT_STEP * driving_ref[...]
    for member in range(count):
        out_ref[member] = (fresh[member * rows : (member + 1) * rows] + forcing).astype(BF16)


def probe_kernel(rows, columns, count, offset_ref, mixing_ref, probes_ref, observed_ref, *refs):
    x_hbm, (after_ref, count_ref, total_ref, weight_ref), x_refs, sems = refs[:3], refs[3:7], refs[7:10], refs[10]
    copies = start_copies(x_hbm, x_refs, sems)
    members = mixing_ref.shape[0]
    for m in range(count):
        weights = [mixing_ref[j, offset_ref[0] + m] for j in range(members)]
        share = (1.0 - state_sum_of(weights)) * (1.0 / members)
        for j in range(members):
            weight_ref[pl.ds(m * members + j, 1), :] = jnp.full((1, columns), weights[j] + share, F32)
    probes = probes_ref[...]
    observed = observed_ref[...]
    amount = probes.shape[1]
    row, column = lax.div(probes, columns), lax.rem(probes, columns)
    in_row = lax.broadcasted_iota(jnp.int32, (rows, amount), 0) == row
    in_column = (lax.broadcasted_iota(jnp.int32, (columns, amount), 0) == column).astype(F32).astype(BF16)
    first = observed.astype(BF16)
    rest = observed - first.astype(F32)
    second = rest.astype(BF16)
    third = (rest - second.astype(F32)).astype(BF16)
    left = [in_row.astype(F32)]
    left += [jnp.where(in_row, piece.astype(F32), 0.0) for piece in (first, second, third)]
    left = jnp.concatenate(left, 0).astype(BF16)
    out = lax.dot_general(left, in_column, NT, preferred_element_type=F32)
    count_ref[...] = out[:rows]
    total_ref[...] = out[rows : 2 * rows] + (out[2 * rows : 3 * rows] + out[3 * rows :])
    for copy in copies:
        copy.wait()


def state_sum_of(values):
    total = values[0]
    for value in values[1:]:
        total = total + value
    return total


def analysis_kernel(values_ref, weight_ref, number_ref, total_ref, out_ref, part_ref, row_ref):
    members, rows, columns = values_ref.shape
    values = [values_ref[j].astype(F32) for j in range(members)]
    for m in range(out_ref.shape[0]):
        at = m * members
        acc = weight_ref[at : at + 1, :] * values[0]
        for j in range(1, members):
            acc = acc + weight_ref[at + j : at + j + 1, :] * values[j]
        out_ref[m] = acc
    number = number_ref[...]
    centre = state_sum_of(values) * (1.0 / members)
    surprise = total_ref[...] - number * centre

    def to_row(product):
        short = product[:, :LANES]
        for at in range(LANES, columns, LANES):
            short = short + product[:, at : at + LANES]
        return jnp.sum(short, 0, keepdims=True)

    anomaly = [v - centre for v in values]
    for i in range(members):
        weighted = anomaly[i] * number
        for j in range(i + 1):
            row = to_row(weighted * anomaly[j])
            row_ref[j, pl.ds(i, 1), :] = row
            if j != i:
                row_ref[i, pl.ds(j, 1), :] = row
        row_ref[members, pl.ds(i, 1), :] = to_row(anomaly[i] * surprise)
    lane = lax.broadcasted_iota(jnp.int32, (members, LANES), 1)
    tile = jnp.zeros((members, LANES), F32)
    for j in range(members + 1):
        tile = jnp.where(lane == j, jnp.sum(row_ref[j], 1, keepdims=True), tile)
    for peer in range(part_ref.shape[0]):
        part_ref[peer] = tile


def total_kernel(probes, parts_ref, spread_ref, projection_ref):
    copies, members, lanes = parts_ref.shape
    total = parts_ref[0]
    for s in range(1, copies):
        total = total + parts_ref[s]
    spread_ref[...] = total[:, :members] * (1.0 / probes)
    lane = lax.broadcasted_iota(jnp.int32, (members, lanes), 1)
    row = lax.broadcasted_iota(jnp.int32, (members, lanes), 0)
    column = jnp.where(lane == row, total[:, members : members + 1], 0.0)
    projection_ref[...] = jnp.sum(column, 0, keepdims=True)[:, :members] * (1.0 / math.sqrt(probes))


VMEM = pl.BlockSpec(memory_space=pltpu.VMEM)
SMEM = pl.BlockSpec(memory_space=pltpu.SMEM)
HBM = pl.BlockSpec(memory_space=pltpu.HBM)


def local(kernel, name, limit, in_specs, out_shape, scratch=()):
    return pl.pallas_call(
        kernel,
        out_shape=out_shape,
        in_specs=in_specs,
        out_specs=jax.tree.map(lambda _: VMEM, out_shape),
        scratch_shapes=scratch,
        compiler_params=pltpu.CompilerParams(vmem_limit_bytes=limit * MIB),
        name=name,
    )


def on_device(plan, participant_swirls, driving_source, mixing, probes, observed):
    count, rows, n = participant_swirls.shape
    members, space = mixing.shape[0], plan.space
    array = jax.ShapeDtypeStruct
    me = lax.axis_index("space").astype(jnp.int32).reshape(1)
    offset = (lax.axis_index("member") * count).astype(jnp.int32).reshape(1)
    group = plan.group
    exchange = functools.partial(lax.all_to_all, axis_name="space", split_axis=0, concat_axis=0, tiled=True)

    def from_peer(value, away):
        return lax.ppermute(value, "space", [(d, d ^ away) for d in range(space)])

    in_hbm = lambda x: pltpu.with_memory_space_constraint(x, pltpu.HBM)
    block_shape = (plan.modes, 2 * rows)
    table = pltpu.VMEM(plan.y_table[0].shape, BF16)
    sent = local(
        functools.partial(rows_kernel, plan), "rows_to_modes", 8, [SMEM] + [HBM] * 4,
        [array(block_shape, F32)] * count,
        [pltpu.VMEM((count * rows, n), F32), table, table, table,
         pltpu.VMEM((count,) + block_shape, F32), pltpu.SemaphoreType.DMA((4,))],
    )(me, *map(in_hbm, (participant_swirls.reshape(count * rows, n), *plan.y_table)))
    blocks = []
    for side in range(count):
        base = sent[0] if side == 0 else from_peer(sent[side], side * group)
        blocks += [base] + [from_peer(base, away) for away in range(1, group)]
    number, total, weights, *x_table = local(
        functools.partial(probe_kernel, rows, n, count), "probe_cells", 16,
        [SMEM, SMEM, VMEM, VMEM] + [HBM] * 3 + [pl.BlockSpec(memory_space=pl.ANY)],
        [array((rows, n), F32), array((rows, n), F32), array((count * members, n), F32)]
        + [array(t.shape, BF16) for t in plan.x_table],
        [pltpu.SemaphoreType.DMA((3,))],
    )(offset, mixing, probes.reshape(1, -1), observed.reshape(1, -1), *map(in_hbm, plan.x_table), blocks[1])
    line = local(
        functools.partial(member_kernel, plan), "member_step", 24, [SMEM] + [HBM] * 3 + [VMEM] * (3 + space),
        array((space, plan.block, 2 * rows), F32),
        [pltpu.VMEM((space,) + block_shape, F32), pltpu.VMEM(plan.y_inverse.shape, BF16),
         pltpu.VMEM(plan.y_own.shape[1:], BF16), pltpu.VMEM(plan.x_inverse.shape, BF16),
         pltpu.VMEM((4, plan.modes, plan.kpad), F32), pltpu.SemaphoreType.DMA((3,))],
    )(me, *map(in_hbm, (plan.y_inverse, plan.y_own, plan.x_inverse)), *x_table, *blocks)
    moved = exchange(line)
    rounded = local(
        functools.partial(finish_kernel, plan), "modes_to_rows", 8, [VMEM] * 5, array((count, rows, n), BF16)
    )(moved, driving_source, *plan.y_table)
    values = lax.all_gather(rounded, "member", axis=0, tiled=True)
    analysis, part = local(
        analysis_kernel, "analysis", 16, [VMEM] * 4,
        [array((count, rows, n), F32), array((space, members, LANES), F32)],
        [pltpu.VMEM((members + 1, members, LANES), F32)],
    )(values, weights, number, total)
    parts = exchange(part)
    spread, projection = local(
        functools.partial(total_kernel, probes.shape[0] * space), "probe_totals", 4, [VMEM],
        [array((members, members), F32), array((1, members), F32)],
    )(parts)
    return analysis, spread, projection.reshape(members)


def solution(mesh):
    space = mesh.shape["space"]

    def body(participant_swirls, *rest):
        count, rows, n = participant_swirls.shape
        return on_device(Plan(n, rows, space, count), participant_swirls, *rest)

    return jax.shard_map(
        body,
        mesh=mesh,
        in_specs=(P("member", "space", None), P("space", None), P(), P("space"), P("space")),
        out_specs=(P("member", "space", None), P(), P()),
        check_vma=False,
    )
```

```python
import functools
import math

import jax
import jax.numpy as jnp
import numpy as np
from jax import lax
from jax.experimental import pallas as pl
from jax.experimental.pallas import tpu as pltpu
from jax.sharding import PartitionSpec as P

KEEP = 160
DT_STEP = 0.1
VISCOSITY = 0.05
LANES = 128
F32 = jnp.float32
BF16 = jnp.bfloat16

NN = (((1,), (0,)), ((), ()))
NT = (((1,), (1,)), ((), ()))
FULL = ((0, 0), (0, 1), (1, 0), (1, 1), (0, 2), (2, 0))
SHORT = ((0, 0), (0, 1), (1, 0))
MIB = 1 << 20
SHORT_ROWS = 128


def round_up(value, unit):
    return -(-value // unit) * unit


def split_table(table, pieces):
    rest, out = np.asarray(table, np.float64), []
    for _ in range(pieces):
        out.append(rest.astype(np.float32).astype(BF16))
        rest = rest - out[-1].astype(np.float64)
    return tuple(jnp.asarray(piece) for piece in out)


def split(value, pieces):
    out = []
    for piece in range(pieces):
        out.append(value.astype(BF16))
        if piece + 1 < pieces:
            value = value - out[-1].astype(F32)
    return out


def product(left, right, dims, terms):
    rows, out = left[0].shape[0], None
    for j in reversed(range(len(right))):
        picks = [i for i, k in terms if k == j]
        groups = [picks] if rows <= SHORT_ROWS else [[i] for i in reversed(picks)]
        for pick in groups:
            tall = left[pick[0]] if len(pick) == 1 else jnp.concatenate([left[i] for i in pick], 0)
            both = lax.dot_general(tall, right[j], dims, preferred_element_type=F32)
            for at in reversed(range(len(pick))):
                term = both[at * rows : (at + 1) * rows]
                out = term if out is None else out + term
    return out


class Plan:
    def __init__(self, n, rows, space, count):
        self.n, self.rows, self.space, self.count = n, rows, space, count
        self.group = space // count
        self.block = round_up(-(-KEEP // self.group), 8)
        self.modes = self.block * self.group
        self.half = n // 2
        self.kpad = round_up(KEEP + 1, LANES)
        cells = np.arange(n) + 0.5
        scale = 2.0 * math.pi / n
        ky = np.concatenate([np.arange(0, self.modes, 2), np.arange(1, self.modes, 2)])
        live = (ky < KEEP)[:, None]
        angle_y = scale * ky[:, None] * cells[None, :]
        waves_y = np.stack([np.cos(angle_y) * live, -np.sin(angle_y) * live])
        self.y_table = split_table(waves_y[:, :, : self.half].reshape(2 * self.modes, self.half), 3)
        quarter = waves_y[:, :, : n // 4]
        self.quarter = n // 4
        high, low = split_table(quarter.reshape(2, 2, self.modes // 2, n // 4).transpose(0, 1, 3, 2), 2)
        self.y_inverse = jnp.concatenate([high, high, low], -1)
        own = 2.0 * quarter.reshape(2, self.group, self.block, n // 4).transpose(1, 0, 2, 3)
        high, low = split_table(own, 2)
        self.y_own = jnp.concatenate(
            [jnp.concatenate([high, high], -1), jnp.concatenate([low, jnp.zeros_like(low)], -1)], -2
        )
        kx = np.arange(self.kpad)
        angle_x = scale * cells[: self.half, None] * kx[None, :]
        keep_x = (kx <= KEEP)[None, :]
        self.x_table = split_table(np.concatenate([np.cos(angle_x) * keep_x, np.sin(angle_x) * keep_x], 1), 3)
        self.main = self.kpad - LANES
        self.step = round_up(KEEP + 1 - self.main, 8)
        high, low = (table.reshape(self.half, 2, self.kpad).transpose(1, 2, 0) for table in self.x_table[:2])
        tails = [table[:, self.main : self.main + self.step] for table in (high, high, low)]
        empty = jnp.zeros((2, LANES - 3 * self.step, self.half), BF16)
        self.x_inverse = jnp.concatenate([t[:, : self.main] for t in (high, high, low)] + tails + [empty], 1)


def reversed_lanes(value):
    width = value.shape[1]
    swap = lax.broadcasted_iota(jnp.int32, (width, width), 0) + lax.broadcasted_iota(jnp.int32, (width, width), 1)
    swap = jnp.where(swap == width - 1, 1.0, 0.0).astype(BF16)
    return product(split(value, 3), [swap], NN, ((0, 0), (1, 0), (2, 0)))


def start_copies(sources, targets, sems):
    copies = [pltpu.make_async_copy(s, t, sems.at[i]) for i, (s, t) in enumerate(zip(sources, targets))]
    for copy in copies:
        copy.start()
    return copies


def rows_kernel(plan, me_ref, field_hbm, y0_hbm, y1_hbm, y2_hbm, *refs):
    rows, modes, count, half = plan.rows, plan.modes, plan.count, plan.half
    outs, (field_ref, y0_ref, y1_ref, y2_ref, packed_ref, sems) = refs[:count], refs[count:]
    copies = start_copies((field_hbm, y0_hbm, y1_hbm, y2_hbm), (field_ref, y0_ref, y1_ref, y2_ref), sems)
    copies[0].wait()
    near, far = field_ref[:, :half], field_ref[:, half:]
    folded = (split(near + far, 3), split(near - far, 3))
    for copy in copies[1:]:
        copy.wait()
    sums = []
    for parity in range(2):
        at = parity * (modes // 2)
        tables = [
            jnp.concatenate([ref[at : at + modes // 2], ref[modes + at : modes + at + modes // 2]], 0)
            for ref in (y0_ref, y1_ref, y2_ref)
        ]
        sums.append(product(tables, folded[parity], NT, FULL))
    real = jnp.concatenate([part[: modes // 2] for part in sums], 0)
    imag = jnp.concatenate([part[modes // 2 :] for part in sums], 0)
    for member in range(count):
        at = slice(member * rows, (member + 1) * rows)
        packed_ref[member] = jnp.concatenate([real[:, at], imag[:, at]], 1)
    side = me_ref[0] // plan.group
    for away in range(count):
        outs[away][...] = packed_ref[side ^ away]


def project(plan, k_lane, cos_re, cos_im, sin_re, sin_im):
    weight = jnp.where((k_lane == 0) | (k_lane == KEEP), 1.0, 2.0)
    edge = jnp.where(k_lane == KEEP, 1.0, 0.0)
    return (
        weight * cos_re - edge * sin_im,
        weight * cos_im + edge * sin_re,
        weight * sin_re + edge * cos_im,
        weight * sin_im - edge * cos_re,
    )


def pack_lines(plan, value):
    high, low = split(value, 2)
    main = [piece[:, : plan.main] for piece in (high, low, high)]
    last_high, last_low = (piece[:, plan.main :].astype(F32) for piece in (high, low))
    tail = last_high + pltpu.roll(last_low, plan.step, 1) + pltpu.roll(last_high, 2 * plan.step, 1)
    return jnp.concatenate(main + [tail.astype(BF16)], 1)


def member_kernel(plan, me_ref, inverse_hbm, own_hbm, lines_hbm, x0_ref, x1_ref, x2_ref, *refs):
    blocks, out_ref, moved_ref = refs[: plan.space], refs[plan.space], refs[plan.space + 1]
    inverse_ref, own_ref, lines_ref, coef_ref, sems = refs[plan.space + 2 :]
    me = me_ref[0]
    own = me % plan.group
    copies = start_copies((inverse_hbm, own_hbm.at[own], lines_hbm), (inverse_ref, own_ref, lines_ref), sems)
    for away in range(plan.space):
        moved_ref[me ^ away] = blocks[away][...]
    n, half, modes, block, kpad, rows = plan.n, plan.half, plan.modes, plan.block, plan.kpad, plan.rows
    unit = 2.0 * math.pi / n
    first = pl.multiple_of(own * block, 8)
    x_refs = (x0_ref, x1_ref, x2_ref)

    def x_cos(pieces):
        return [ref[:, :kpad] for ref in x_refs[:pieces]]

    def x_sin(pieces):
        return [ref[:, kpad:] for ref in x_refs[:pieces]]

    def gathered(lanes, first, last):
        return jnp.concatenate([moved_ref[s, :, lanes] for s in range(first, last)], 1)

    def waves(count, start):
        k_lane = lax.broadcasted_iota(jnp.int32, (count, kpad), 1)
        row = lax.broadcasted_iota(jnp.int32, (count, kpad), 0) + start
        ky_row = jnp.where(row < modes // 2, 2 * row, 2 * row - (modes - 1))
        wave_x = k_lane.astype(F32) * unit
        wave_y = ky_row.astype(F32) * unit
        return k_lane, ky_row, wave_x, wave_y, wave_x * wave_x + wave_y * wave_y

    rows_of = lambda re, im: jnp.concatenate([re, im], 0)
    parts_of = lambda first, last: rows_of(
        gathered(slice(0, rows), first, last), gathered(slice(rows, 2 * rows), first, last)
    )
    near = parts_of(0, plan.space // 2)
    far = reversed_lanes(parts_of(plan.space // 2, plan.space))
    cos_sums = product(split(near + far, 3), x_cos(3), NN, FULL)
    sin_sums = product(split(near - far, 3), x_sin(3), NN, FULL)
    sums = (cos_sums[:modes], cos_sums[modes:], sin_sums[:modes], sin_sums[modes:])
    for part in range(4):
        coef_ref[part] = sums[part]
    k_lane, ky_row, wave_x, wave_y, squared = waves(modes, 0)
    live = squared > 0
    inverse_sq = jnp.where(live, 1.0 / jnp.where(live, squared, 1.0), 0.0)
    weight = jnp.where(ky_row == 0, 1.0 / (n * n), 2.0 / (n * n))
    a_re, a_im, b_re, b_im = project(plan, k_lane, *[s * weight for s in sums])
    pa_re, pa_im, pb_re, pb_im = (c * inverse_sq for c in (a_re, a_im, b_re, b_im))
    copies[0].wait()
    copies[2].wait()

    def along_quarter(part, lines):
        out = []
        for parity in range(2):
            high, low = split(lines[parity * (modes // 2) : (parity + 1) * (modes // 2)], 2)
            out.append(
                lax.dot_general(
                    inverse_ref[part, parity], jnp.concatenate([high, low, high], 0), NN, preferred_element_type=F32
                )
            )
        return out

    def to_cells(cos_part, sin_part):
        even = lax.dot_general(pack_lines(plan, cos_part), lines_ref[0], NN, preferred_element_type=F32)
        odd = lax.dot_general(pack_lines(plan, sin_part), lines_ref[1], NN, preferred_element_type=F32)
        both = jnp.concatenate([even + odd, even - odd], 1)
        cos_a, cos_b = along_quarter(0, both[:modes])
        sin_a, sin_b = along_quarter(1, both[modes:])
        return (cos_a + cos_b, cos_a - cos_b), (sin_b + sin_a, sin_b - sin_a)

    def along_x(cos_re, cos_im, sin_re, sin_im):
        return to_cells(
            rows_of(wave_x * sin_re, wave_x * sin_im), rows_of(-wave_x * cos_re, -wave_x * cos_im)
        )

    def along_y(cos_re, cos_im, sin_re, sin_im):
        return to_cells(
            rows_of(-wave_y * cos_im, wave_y * cos_re), rows_of(-wave_y * sin_im, wave_y * sin_re)
        )

    w_modes, p_modes = (a_re, a_im, b_re, b_im), (pa_re, pa_im, pb_re, pb_im)
    even, odd = [0.0, 0.0], [0.0, 0.0]
    for flow, slope, sign in ((along_y(*p_modes), along_x(*w_modes), 1.0), (along_x(*p_modes), along_y(*w_modes), -1.0)):
        (flow_cos, flow_sin), (slope_cos, slope_sin) = flow, slope
        for at in range(2):
            even[at] = even[at] + sign * (flow_cos[at] * slope_cos[at] + flow_sin[at] * slope_sin[at])
            odd[at] = odd[at] + sign * (flow_cos[at] * slope_sin[at] + flow_sin[at] * slope_cos[at])

    copies[1].wait()
    mirror = jnp.where(own < plan.group // 2, 1.0, -1.0)

    def own_modes(part, folded):
        both = lax.dot_general(
            own_ref[part], jnp.concatenate(split(folded, 2), 0), NN, preferred_element_type=F32
        )
        return both[:block] + both[block:]

    hats = rows_of(own_modes(0, even[0] + mirror * even[1]), own_modes(1, odd[0] - mirror * odd[1]))
    hat_cos = product(split(hats[:, :half] + hats[:, half:], 2), x_cos(2), NN, SHORT)
    hat_sin = product(split(hats[:, :half] - hats[:, half:], 2), x_sin(2), NN, SHORT)
    advect = (hat_cos[:block], hat_cos[block:], hat_sin[:block], hat_sin[block:])

    mine = [coef_ref[part, pl.ds(first, block), :] for part in range(4)]
    k_lane, _, _, _, squared = waves(block, first)
    fade = 1.0 - (DT_STEP * VISCOSITY) * squared
    new = project(plan, k_lane, *[m * fade - DT_STEP * q for m, q in zip(mine, advect)])
    even = product(split(rows_of(new[0], new[1]), 3), x_cos(3), NT, FULL)
    odd = product(split(rows_of(new[2], new[3]), 3), x_sin(3), NT, FULL)
    line = jnp.concatenate([even + odd, reversed_lanes(even - odd)], 1)
    for peer in range(plan.space):
        cut = slice(peer * rows, (peer + 1) * rows)
        out_ref[peer] = jnp.concatenate([line[:block, cut], line[block:, cut]], 1)


def finish_kernel(plan, moved_ref, driving_ref, y0_ref, y1_ref, y2_ref, out_ref):
    rows, modes, n, count = plan.rows, plan.modes, plan.n, plan.count
    ky = lax.broadcasted_iota(jnp.int32, (modes, 2 * rows), 0)
    weight = jnp.where(ky == 0, 1.0 / (n * n), 2.0 / (n * n))
    lines = []
    for member in range(count):
        line = moved_ref[member * plan.group : (member + 1) * plan.group].reshape(modes, 2 * rows)
        lines.append(jnp.transpose(line * weight))
    real = jnp.concatenate([line[:rows] for line in lines], 0)
    imag = jnp.concatenate([line[rows:] for line in lines], 0)
    y_refs = (y0_ref, y1_ref, y2_ref)
    even = product(split(real, 3), [ref[:modes] for ref in y_refs], NN, FULL)
    odd = product(split(imag, 3), [ref[modes:] for ref in y_refs], NN, FULL)
    fresh = jnp.concatenate([even + odd, reversed_lanes(even - odd)], 1)
    forcing = DT_STEP * driving_ref[...]
    for member in range(count):
        out_ref[member] = (fresh[member * rows : (member + 1) * rows] + forcing).astype(BF16)


def probe_kernel(rows, columns, count, offset_ref, mixing_ref, probes_ref, observed_ref, *refs):
    x_hbm, (after_ref, count_ref, total_ref, weight_ref), x_refs, sems = refs[:3], refs[3:7], refs[7:10], refs[10]
    copies = start_copies(x_hbm, x_refs, sems)
    members = mixing_ref.shape[0]
    for m in range(count):
        weights = [mixing_ref[j, offset_ref[0] + m] for j in range(members)]
        share = (1.0 - state_sum_of(weights)) * (1.0 / members)
        for j in range(members):
            weight_ref[pl.ds(m * members + j, 1), :] = jnp.full((1, columns), weights[j] + share, F32)
    probes = probes_ref[...]
    observed = observed_ref[...]
    amount = probes.shape[1]
    row, column = lax.div(probes, columns), lax.rem(probes, columns)
    in_row = lax.broadcasted_iota(jnp.int32, (rows, amount), 0) == row
    in_column = (lax.broadcasted_iota(jnp.int32, (columns, amount), 0) == column).astype(F32).astype(BF16)
    first = observed.astype(BF16)
    rest = observed - first.astype(F32)
    second = rest.astype(BF16)
    third = (rest - second.astype(F32)).astype(BF16)
    left = [in_row.astype(F32)]
    left += [jnp.where(in_row, piece.astype(F32), 0.0) for piece in (first, second, third)]
    left = jnp.concatenate(left, 0).astype(BF16)
    out = lax.dot_general(left, in_column, NT, preferred_element_type=F32)
    count_ref[...] = out[:rows]
    total_ref[...] = out[rows : 2 * rows] + (out[2 * rows : 3 * rows] + out[3 * rows :])
    for copy in copies:
        copy.wait()


def state_sum_of(values):
    total = values[0]
    for value in values[1:]:
        total = total + value
    return total


def analysis_kernel(values_ref, weight_ref, number_ref, total_ref, out_ref, part_ref, row_ref):
    members, rows, columns = values_ref.shape
    values = [values_ref[j].astype(F32) for j in range(members)]
    for m in range(out_ref.shape[0]):
        at = m * members
        acc = weight_ref[at : at + 1, :] * values[0]
        for j in range(1, members):
            acc = acc + weight_ref[at + j : at + j + 1, :] * values[j]
        out_ref[m] = acc
    number = number_ref[...]
    centre = state_sum_of(values) * (1.0 / members)
    surprise = total_ref[...] - number * centre

    def to_row(product):
        short = product[:, :LANES]
        for at in range(LANES, columns, LANES):
            short = short + product[:, at : at + LANES]
        return jnp.sum(short, 0, keepdims=True)

    anomaly = [v - centre for v in values]
    for i in range(members):
        weighted = anomaly[i] * number
        for j in range(i + 1):
            row = to_row(weighted * anomaly[j])
            row_ref[j, pl.ds(i, 1), :] = row
            if j != i:
                row_ref[i, pl.ds(j, 1), :] = row
        row_ref[members, pl.ds(i, 1), :] = to_row(anomaly[i] * surprise)
    lane = lax.broadcasted_iota(jnp.int32, (members, LANES), 1)
    tile = jnp.zeros((members, LANES), F32)
    for j in range(members + 1):
        tile = jnp.where(lane == j, jnp.sum(row_ref[j], 1, keepdims=True), tile)
    for peer in range(part_ref.shape[0]):
        part_ref[peer] = tile


def total_kernel(probes, parts_ref, spread_ref, projection_ref):
    copies, members, lanes = parts_ref.shape
    total = parts_ref[0]
    for s in range(1, copies):
        total = total + parts_ref[s]
    spread_ref[...] = total[:, :members] * (1.0 / probes)
    lane = lax.broadcasted_iota(jnp.int32, (members, lanes), 1)
    row = lax.broadcasted_iota(jnp.int32, (members, lanes), 0)
    column = jnp.where(lane == row, total[:, members : members + 1], 0.0)
    projection_ref[...] = jnp.sum(column, 0, keepdims=True)[:, :members] * (1.0 / math.sqrt(probes))


VMEM = pl.BlockSpec(memory_space=pltpu.VMEM)
SMEM = pl.BlockSpec(memory_space=pltpu.SMEM)
HBM = pl.BlockSpec(memory_space=pltpu.HBM)


def local(kernel, name, limit, in_specs, out_shape, scratch=()):
    return pl.pallas_call(
        kernel,
        out_shape=out_shape,
        in_specs=in_specs,
        out_specs=jax.tree.map(lambda _: VMEM, out_shape),
        scratch_shapes=scratch,
        compiler_params=pltpu.CompilerParams(vmem_limit_bytes=limit * MIB),
        name=name,
    )


def on_device(plan, participant_swirls, driving_source, mixing, probes, observed):
    count, rows, n = participant_swirls.shape
    members, space = mixing.shape[0], plan.space
    array = jax.ShapeDtypeStruct
    me = lax.axis_index("space").astype(jnp.int32).reshape(1)
    offset = (lax.axis_index("member") * count).astype(jnp.int32).reshape(1)
    group = plan.group
    exchange = functools.partial(lax.all_to_all, axis_name="space", split_axis=0, concat_axis=0, tiled=True)

    def from_peer(value, away):
        return lax.ppermute(value, "space", [(d, d ^ away) for d in range(space)])

    in_hbm = lambda x: pltpu.with_memory_space_constraint(x, pltpu.HBM)
    block_shape = (plan.modes, 2 * rows)
    table = pltpu.VMEM(plan.y_table[0].shape, BF16)
    sent = local(
        functools.partial(rows_kernel, plan), "rows_to_modes", 8, [SMEM] + [HBM] * 4,
        [array(block_shape, F32)] * count,
        [pltpu.VMEM((count * rows, n), F32), table, table, table,
         pltpu.VMEM((count,) + block_shape, F32), pltpu.SemaphoreType.DMA((4,))],
    )(me, *map(in_hbm, (participant_swirls.reshape(count * rows, n), *plan.y_table)))
    blocks = []
    for side in range(count):
        base = sent[0] if side == 0 else from_peer(sent[side], side * group)
        blocks += [base] + [from_peer(base, away) for away in range(1, group)]
    number, total, weights, *x_table = local(
        functools.partial(probe_kernel, rows, n, count), "probe_cells", 16,
        [SMEM, SMEM, VMEM, VMEM] + [HBM] * 3 + [pl.BlockSpec(memory_space=pl.ANY)],
        [array((rows, n), F32), array((rows, n), F32), array((count * members, n), F32)]
        + [array(t.shape, BF16) for t in plan.x_table],
        [pltpu.SemaphoreType.DMA((3,))],
    )(offset, mixing, probes.reshape(1, -1), observed.reshape(1, -1), *map(in_hbm, plan.x_table), blocks[1])
    line = local(
        functools.partial(member_kernel, plan), "member_step", 24, [SMEM] + [HBM] * 3 + [VMEM] * (3 + space),
        array((space, plan.block, 2 * rows), F32),
        [pltpu.VMEM((space,) + block_shape, F32), pltpu.VMEM(plan.y_inverse.shape, BF16),
         pltpu.VMEM(plan.y_own.shape[1:], BF16), pltpu.VMEM(plan.x_inverse.shape, BF16),
         pltpu.VMEM((4, plan.modes, plan.kpad), F32), pltpu.SemaphoreType.DMA((3,))],
    )(me, *map(in_hbm, (plan.y_inverse, plan.y_own, plan.x_inverse)), *x_table, *blocks)
    moved = exchange(line)
    rounded = local(
        functools.partial(finish_kernel, plan), "modes_to_rows", 8, [VMEM] * 5, array((count, rows, n), BF16)
    )(moved, driving_source, *plan.y_table)
    values = lax.all_gather(rounded, "member", axis=0, tiled=True)
    analysis, part = local(
        analysis_kernel, "analysis", 16, [VMEM] * 4,
        [array((count, rows, n), F32), array((space, members, LANES), F32)],
        [pltpu.VMEM((members + 1, members, LANES), F32)],
    )(values, weights, number, total)
    parts = exchange(part)
    spread, projection = local(
        functools.partial(total_kernel, probes.shape[0] * space), "probe_totals", 4, [VMEM],
        [array((members, members), F32), array((1, members), F32)],
    )(parts)
    return analysis, spread, projection.reshape(members)


def solution(mesh):
    space = mesh.shape["space"]

    def body(participant_swirls, *rest):
        count, rows, n = participant_swirls.shape
        return on_device(Plan(n, rows, space, count), participant_swirls, *rest)

    return jax.shard_map(
        body,
        mesh=mesh,
        in_specs=(P("member", "space", None), P("space", None), P(), P("space"), P("space")),
        out_specs=(P("member", "space", None), P(), P()),
        check_vma=False,
    )
```

```python
import functools
import math

import jax
import jax.numpy as jnp
import numpy as np
from jax import lax
from jax.experimental import pallas as pl
from jax.experimental.pallas import tpu as pltpu
from jax.sharding import PartitionSpec as P

KEEP = 160
DT_STEP = 0.1
VISCOSITY = 0.05
LANES = 128
F32 = jnp.float32
BF16 = jnp.bfloat16

NN = (((1,), (0,)), ((), ()))
NT = (((1,), (1,)), ((), ()))
FULL = ((0, 0), (0, 1), (1, 0), (1, 1), (0, 2), (2, 0))
SHORT = ((0, 0), (0, 1), (1, 0))
MIB = 1 << 20
SHORT_ROWS = 128


def round_up(value, unit):
    return -(-value // unit) * unit


def split_table(table, pieces):
    rest, out = np.asarray(table, np.float64), []
    for _ in range(pieces):
        out.append(rest.astype(np.float32).astype(BF16))
        rest = rest - out[-1].astype(np.float64)
    return tuple(jnp.asarray(piece) for piece in out)


def split(value, pieces):
    out = []
    for piece in range(pieces):
        out.append(value.astype(BF16))
        if piece + 1 < pieces:
            value = value - out[-1].astype(F32)
    return out


def product(left, right, dims, terms):
    rows, out = left[0].shape[0], None
    for j in reversed(range(len(right))):
        picks = [i for i, k in terms if k == j]
        groups = [picks] if rows <= SHORT_ROWS else [[i] for i in reversed(picks)]
        for pick in groups:
            tall = left[pick[0]] if len(pick) == 1 else jnp.concatenate([left[i] for i in pick], 0)
            both = lax.dot_general(tall, right[j], dims, preferred_element_type=F32)
            for at in reversed(range(len(pick))):
                term = both[at * rows : (at + 1) * rows]
                out = term if out is None else out + term
    return out


class Plan:
    def __init__(self, n, rows, space, count):
        self.n, self.rows, self.space, self.count = n, rows, space, count
        self.group = space // count
        self.block = round_up(-(-KEEP // self.group), 8)
        self.modes = self.block * self.group
        self.half = n // 2
        self.kpad = round_up(KEEP + 1, LANES)
        cells = np.arange(n) + 0.5
        scale = 2.0 * math.pi / n
        ky = np.concatenate([np.arange(0, self.modes, 2), np.arange(1, self.modes, 2)])
        live = (ky < KEEP)[:, None]
        angle_y = scale * ky[:, None] * cells[None, :]
        waves_y = np.stack([np.cos(angle_y) * live, -np.sin(angle_y) * live])
        self.y_table = split_table(waves_y[:, :, : self.half].reshape(2 * self.modes, self.half), 3)
        quarter = waves_y[:, :, : n // 4]
        self.quarter = n // 4
        high, low = split_table(quarter.reshape(2, 2, self.modes // 2, n // 4).transpose(0, 1, 3, 2), 2)
        self.y_inverse = jnp.concatenate([high, high, low], -1)
        own = 2.0 * quarter.reshape(2, self.group, self.block, n // 4).transpose(1, 0, 2, 3)
        high, low = split_table(own, 2)
        self.y_own = jnp.concatenate(
            [jnp.concatenate([high, high], -1), jnp.concatenate([low, jnp.zeros_like(low)], -1)], -2
        )
        kx = np.arange(self.kpad)
        angle_x = scale * cells[: self.half, None] * kx[None, :]
        keep_x = (kx <= KEEP)[None, :]
        self.x_table = split_table(np.concatenate([np.cos(angle_x) * keep_x, np.sin(angle_x) * keep_x], 1), 3)
        self.main = self.kpad - LANES
        self.step = round_up(KEEP + 1 - self.main, 8)
        high, low = (table.reshape(self.half, 2, self.kpad).transpose(1, 2, 0) for table in self.x_table[:2])
        tails = [table[:, self.main : self.main + self.step] for table in (high, high, low)]
        empty = jnp.zeros((2, LANES - 3 * self.step, self.half), BF16)
        self.x_inverse = jnp.concatenate([t[:, : self.main] for t in (high, high, low)] + tails + [empty], 1)


def reversed_lanes(value):
    width = value.shape[1]
    swap = lax.broadcasted_iota(jnp.int32, (width, width), 0) + lax.broadcasted_iota(jnp.int32, (width, width), 1)
    swap = jnp.where(swap == width - 1, 1.0, 0.0).astype(BF16)
    return product(split(value, 3), [swap], NN, ((0, 0), (1, 0), (2, 0)))


def start_copies(sources, targets, sems):
    copies = [pltpu.make_async_copy(s, t, sems.at[i]) for i, (s, t) in enumerate(zip(sources, targets))]
    for copy in copies:
        copy.start()
    return copies


def rows_kernel(plan, me_ref, field_hbm, y0_hbm, y1_hbm, y2_hbm, *refs):
    rows, modes, count, half = plan.rows, plan.modes, plan.count, plan.half
    outs, (field_ref, y0_ref, y1_ref, y2_ref, packed_ref, sems) = refs[:count], refs[count:]
    copies = start_copies((field_hbm, y0_hbm, y1_hbm, y2_hbm), (field_ref, y0_ref, y1_ref, y2_ref), sems)
    copies[0].wait()
    near, far = field_ref[:, :half], field_ref[:, half:]
    folded = (split(near + far, 3), split(near - far, 3))
    for copy in copies[1:]:
        copy.wait()
    sums = []
    for parity in range(2):
        at = parity * (modes // 2)
        tables = [
            jnp.concatenate([ref[at : at + modes // 2], ref[modes + at : modes + at + modes // 2]], 0)
            for ref in (y0_ref, y1_ref, y2_ref)
        ]
        sums.append(product(tables, folded[parity], NT, FULL))
    real = jnp.concatenate([part[: modes // 2] for part in sums], 0)
    imag = jnp.concatenate([part[modes // 2 :] for part in sums], 0)
    for member in range(count):
        at = slice(member * rows, (member + 1) * rows)
        packed_ref[member] = jnp.concatenate([real[:, at], imag[:, at]], 1)
    side = me_ref[0] // plan.group
    for away in range(count):
        outs[away][...] = packed_ref[side ^ away]


def project(plan, k_lane, cos_re, cos_im, sin_re, sin_im):
    weight = jnp.where((k_lane == 0) | (k_lane == KEEP), 1.0, 2.0)
    edge = jnp.where(k_lane == KEEP, 1.0, 0.0)
    return (
        weight * cos_re - edge * sin_im,
        weight * cos_im + edge * sin_re,
        weight * sin_re + edge * cos_im,
        weight * sin_im - edge * cos_re,
    )


def pack_lines(plan, value):
    high, low = split(value, 2)
    main = [piece[:, : plan.main] for piece in (high, low, high)]
    last_high, last_low = (piece[:, plan.main :].astype(F32) for piece in (high, low))
    tail = last_high + pltpu.roll(last_low, plan.step, 1) + pltpu.roll(last_high, 2 * plan.step, 1)
    return jnp.concatenate(main + [tail.astype(BF16)], 1)


def member_kernel(plan, me_ref, inverse_hbm, own_hbm, lines_hbm, x0_ref, x1_ref, x2_ref, *refs):
    blocks, out_ref, moved_ref = refs[: plan.space], refs[plan.space], refs[plan.space + 1]
    inverse_ref, own_ref, lines_ref, coef_ref, sems = refs[plan.space + 2 :]
    me = me_ref[0]
    own = me % plan.group
    copies = start_copies((inverse_hbm, own_hbm.at[own], lines_hbm), (inverse_ref, own_ref, lines_ref), sems)
    for away in range(plan.space):
        moved_ref[me ^ away] = blocks[away][...]
    n, half, modes, block, kpad, rows = plan.n, plan.half, plan.modes, plan.block, plan.kpad, plan.rows
    unit = 2.0 * math.pi / n
    first = pl.multiple_of(own * block, 8)
    x_refs = (x0_ref, x1_ref, x2_ref)

    def x_cos(pieces):
        return [ref[:, :kpad] for ref in x_refs[:pieces]]

    def x_sin(pieces):
        return [ref[:, kpad:] for ref in x_refs[:pieces]]

    def gathered(lanes, first, last):
        return jnp.concatenate([moved_ref[s, :, lanes] for s in range(first, last)], 1)

    def waves(count, start):
        k_lane = lax.broadcasted_iota(jnp.int32, (count, kpad), 1)
        row = lax.broadcasted_iota(jnp.int32, (count, kpad), 0) + start
        ky_row = jnp.where(row < modes // 2, 2 * row, 2 * row - (modes - 1))
        wave_x = k_lane.astype(F32) * unit
        wave_y = ky_row.astype(F32) * unit
        return k_lane, ky_row, wave_x, wave_y, wave_x * wave_x + wave_y * wave_y

    rows_of = lambda re, im: jnp.concatenate([re, im], 0)
    parts_of = lambda first, last: rows_of(
        gathered(slice(0, rows), first, last), gathered(slice(rows, 2 * rows), first, last)
    )
    near = parts_of(0, plan.space // 2)
    far = reversed_lanes(parts_of(plan.space // 2, plan.space))
    cos_sums = product(split(near + far, 3), x_cos(3), NN, FULL)
    sin_sums = product(split(near - far, 3), x_sin(3), NN, FULL)
    sums = (cos_sums[:modes], cos_sums[modes:], sin_sums[:modes], sin_sums[modes:])
    for part in range(4):
        coef_ref[part] = sums[part]
    k_lane, ky_row, wave_x, wave_y, squared = waves(modes, 0)
    live = squared > 0
    inverse_sq = jnp.where(live, 1.0 / jnp.where(live, squared, 1.0), 0.0)
    weight = jnp.where(ky_row == 0, 1.0 / (n * n), 2.0 / (n * n))
    a_re, a_im, b_re, b_im = project(plan, k_lane, *[s * weight for s in sums])
    pa_re, pa_im, pb_re, pb_im = (c * inverse_sq for c in (a_re, a_im, b_re, b_im))
    copies[0].wait()
    copies[2].wait()

    def along_quarter(part, lines):
        out = []
        for parity in range(2):
            high, low = split(lines[parity * (modes // 2) : (parity + 1) * (modes // 2)], 2)
            out.append(
                lax.dot_general(
                    inverse_ref[part, parity], jnp.concatenate([high, low, high], 0), NN, preferred_element_type=F32
                )
            )
        return out

    def to_cells(cos_part, sin_part):
        even = lax.dot_general(pack_lines(plan, cos_part), lines_ref[0], NN, preferred_element_type=F32)
        odd = lax.dot_general(pack_lines(plan, sin_part), lines_ref[1], NN, preferred_element_type=F32)
        both = jnp.concatenate([even + odd, even - odd], 1)
        cos_a, cos_b = along_quarter(0, both[:modes])
        sin_a, sin_b = along_quarter(1, both[modes:])
        return (cos_a + cos_b, cos_a - cos_b), (sin_b + sin_a, sin_b - sin_a)

    def along_x(cos_re, cos_im, sin_re, sin_im):
        return to_cells(
            rows_of(wave_x * sin_re, wave_x * sin_im), rows_of(-wave_x * cos_re, -wave_x * cos_im)
        )

    def along_y(cos_re, cos_im, sin_re, sin_im):
        return to_cells(
            rows_of(-wave_y * cos_im, wave_y * cos_re), rows_of(-wave_y * sin_im, wave_y * sin_re)
        )

    w_modes, p_modes = (a_re, a_im, b_re, b_im), (pa_re, pa_im, pb_re, pb_im)
    even, odd = [0.0, 0.0], [0.0, 0.0]
    for flow, slope, sign in ((along_y(*p_modes), along_x(*w_modes), 1.0), (along_x(*p_modes), along_y(*w_modes), -1.0)):
        (flow_cos, flow_sin), (slope_cos, slope_sin) = flow, slope
        for at in range(2):
            even[at] = even[at] + sign * (flow_cos[at] * slope_cos[at] + flow_sin[at] * slope_sin[at])
            odd[at] = odd[at] + sign * (flow_cos[at] * slope_sin[at] + flow_sin[at] * slope_cos[at])

    copies[1].wait()
    mirror = jnp.where(own < plan.group // 2, 1.0, -1.0)

    def own_modes(part, folded):
        both = lax.dot_general(
            own_ref[part], jnp.concatenate(split(folded, 2), 0), NN, preferred_element_type=F32
        )
        return both[:block] + both[block:]

    hats = rows_of(own_modes(0, even[0] + mirror * even[1]), own_modes(1, odd[0] - mirror * odd[1]))
    hat_cos = product(split(hats[:, :half] + hats[:, half:], 2), x_cos(2), NN, SHORT)
    hat_sin = product(split(hats[:, :half] - hats[:, half:], 2), x_sin(2), NN, SHORT)
    advect = (hat_cos[:block], hat_cos[block:], hat_sin[:block], hat_sin[block:])

    mine = [coef_ref[part, pl.ds(first, block), :] for part in range(4)]
    k_lane, _, _, _, squared = waves(block, first)
    fade = 1.0 - (DT_STEP * VISCOSITY) * squared
    new = project(plan, k_lane, *[m * fade - DT_STEP * q for m, q in zip(mine, advect)])
    even = product(split(rows_of(new[0], new[1]), 3), x_cos(3), NT, FULL)
    odd = product(split(rows_of(new[2], new[3]), 3), x_sin(3), NT, FULL)
    line = jnp.concatenate([even + odd, reversed_lanes(even - odd)], 1)
    for peer in range(plan.space):
        cut = slice(peer * rows, (peer + 1) * rows)
        out_ref[peer] = jnp.concatenate([line[:block, cut], line[block:, cut]], 1)


def finish_kernel(plan, moved_ref, driving_ref, y0_ref, y1_ref, y2_ref, out_ref):
    rows, modes, n, count = plan.rows, plan.modes, plan.n, plan.count
    ky = lax.broadcasted_iota(jnp.int32, (modes, 2 * rows), 0)
    weight = jnp.where(ky == 0, 1.0 / (n * n), 2.0 / (n * n))
    lines = []
    for member in range(count):
        line = moved_ref[member * plan.group : (member + 1) * plan.group].reshape(modes, 2 * rows)
        lines.append(jnp.transpose(line * weight))
    real = jnp.concatenate([line[:rows] for line in lines], 0)
    imag = jnp.concatenate([line[rows:] for line in lines], 0)
    y_refs = (y0_ref, y1_ref, y2_ref)
    even = product(split(real, 3), [ref[:modes] for ref in y_refs], NN, FULL)
    odd = product(split(imag, 3), [ref[modes:] for ref in y_refs], NN, FULL)
    fresh = jnp.concatenate([even + odd, reversed_lanes(even - odd)], 1)
    forcing = DT_STEP * driving_ref[...]
    for member in range(count):
        out_ref[member] = (fresh[member * rows : (member + 1) * rows] + forcing).astype(BF16)


def probe_kernel(rows, columns, count, offset_ref, mixing_ref, probes_ref, observed_ref, *refs):
    x_hbm, (after_ref, count_ref, total_ref, weight_ref), x_refs, sems = refs[:3], refs[3:7], refs[7:10], refs[10]
    copies = start_copies(x_hbm, x_refs, sems)
    members = mixing_ref.shape[0]
    for m in range(count):
        weights = [mixing_ref[j, offset_ref[0] + m] for j in range(members)]
        share = (1.0 - state_sum_of(weights)) * (1.0 / members)
        for j in range(members):
            weight_ref[pl.ds(m * members + j, 1), :] = jnp.full((1, columns), weights[j] + share, F32)
    probes = probes_ref[...]
    observed = observed_ref[...]
    amount = probes.shape[1]
    row, column = lax.div(probes, columns), lax.rem(probes, columns)
    in_row = lax.broadcasted_iota(jnp.int32, (rows, amount), 0) == row
    in_column = (lax.broadcasted_iota(jnp.int32, (columns, amount), 0) == column).astype(F32).astype(BF16)
    first = observed.astype(BF16)
    rest = observed - first.astype(F32)
    second = rest.astype(BF16)
    third = (rest - second.astype(F32)).astype(BF16)
    left = [in_row.astype(F32)]
    left += [jnp.where(in_row, piece.astype(F32), 0.0) for piece in (first, second, third)]
    left = jnp.concatenate(left, 0).astype(BF16)
    out = lax.dot_general(left, in_column, NT, preferred_element_type=F32)
    count_ref[...] = out[:rows]
    total_ref[...] = out[rows : 2 * rows] + (out[2 * rows : 3 * rows] + out[3 * rows :])
    for copy in copies:
        copy.wait()


def state_sum_of(values):
    total = values[0]
    for value in values[1:]:
        total = total + value
    return total


def analysis_kernel(values_ref, weight_ref, number_ref, total_ref, out_hbm, part_ref, row_ref, out_ref, sem):
    members, rows, columns = values_ref.shape
    values = [values_ref[j].astype(F32) for j in range(members)]
    for m in range(out_ref.shape[0]):
        at = m * members
        acc = weight_ref[at : at + 1, :] * values[0]
        for j in range(1, members):
            acc = acc + weight_ref[at + j : at + j + 1, :] * values[j]
        out_ref[m] = acc
    copy = pltpu.make_async_copy(out_ref, out_hbm, sem)
    copy.start()
    number = number_ref[...]
    centre = state_sum_of(values) * (1.0 / members)
    surprise = total_ref[...] - number * centre

    def to_row(product):
        short = product[:, :LANES]
        for at in range(LANES, columns, LANES):
            short = short + product[:, at : at + LANES]
        return jnp.sum(short, 0, keepdims=True)

    anomaly = [v - centre for v in values]
    for i in range(members):
        weighted = anomaly[i] * number
        for j in range(i + 1):
            row = to_row(weighted * anomaly[j])
            row_ref[j, pl.ds(i, 1), :] = row
            if j != i:
                row_ref[i, pl.ds(j, 1), :] = row
        row_ref[members, pl.ds(i, 1), :] = to_row(anomaly[i] * surprise)
    lane = lax.broadcasted_iota(jnp.int32, (members, LANES), 1)
    tile = jnp.zeros((members, LANES), F32)
    for j in range(members + 1):
        tile = jnp.where(lane == j, jnp.sum(row_ref[j], 1, keepdims=True), tile)
    for peer in range(part_ref.shape[0]):
        part_ref[peer] = tile
    copy.wait()


def total_kernel(probes, parts_ref, spread_ref, projection_ref):
    copies, members, lanes = parts_ref.shape
    total = parts_ref[0]
    for s in range(1, copies):
        total = total + parts_ref[s]
    spread_ref[...] = total[:, :members] * (1.0 / probes)
    lane = lax.broadcasted_iota(jnp.int32, (members, lanes), 1)
    row = lax.broadcasted_iota(jnp.int32, (members, lanes), 0)
    column = jnp.where(lane == row, total[:, members : members + 1], 0.0)
    projection_ref[...] = jnp.sum(column, 0, keepdims=True)[:, :members] * (1.0 / math.sqrt(probes))


VMEM = pl.BlockSpec(memory_space=pltpu.VMEM)
SMEM = pl.BlockSpec(memory_space=pltpu.SMEM)
HBM = pl.BlockSpec(memory_space=pltpu.HBM)


def local(kernel, name, limit, in_specs, out_shape, scratch=(), out_specs=None):
    return pl.pallas_call(
        kernel,
        out_shape=out_shape,
        in_specs=in_specs,
        out_specs=out_specs or jax.tree.map(lambda _: VMEM, out_shape),
        scratch_shapes=scratch,
        compiler_params=pltpu.CompilerParams(vmem_limit_bytes=limit * MIB),
        name=name,
    )


def on_device(plan, participant_swirls, driving_source, mixing, probes, observed):
    count, rows, n = participant_swirls.shape
    members, space = mixing.shape[0], plan.space
    array = jax.ShapeDtypeStruct
    me = lax.axis_index("space").astype(jnp.int32).reshape(1)
    offset = (lax.axis_index("member") * count).astype(jnp.int32).reshape(1)
    group = plan.group
    exchange = functools.partial(lax.all_to_all, axis_name="space", split_axis=0, concat_axis=0, tiled=True)

    def from_peer(value, away):
        return lax.ppermute(value, "space", [(d, d ^ away) for d in range(space)])

    in_hbm = lambda x: pltpu.with_memory_space_constraint(x, pltpu.HBM)
    block_shape = (plan.modes, 2 * rows)
    table = pltpu.VMEM(plan.y_table[0].shape, BF16)
    sent = local(
        functools.partial(rows_kernel, plan), "rows_to_modes", 8, [SMEM] + [HBM] * 4,
        [array(block_shape, F32)] * count,
        [pltpu.VMEM((count * rows, n), F32), table, table, table,
         pltpu.VMEM((count,) + block_shape, F32), pltpu.SemaphoreType.DMA((4,))],
    )(me, *map(in_hbm, (participant_swirls.reshape(count * rows, n), *plan.y_table)))
    blocks = {}
    for side in range(count):
        turn = side * group + (group // 2 if side else 0)
        blocks[turn] = from_peer(sent[side], turn) if side else sent[0]
        blocks.update({turn ^ away: from_peer(blocks[turn], away) for away in range(1, group)})
    blocks = [blocks[away] for away in range(space)]
    number, total, weights, *x_table = local(
        functools.partial(probe_kernel, rows, n, count), "probe_cells", 16,
        [SMEM, SMEM, VMEM, VMEM] + [HBM] * 3 + [pl.BlockSpec(memory_space=pl.ANY)],
        [array((rows, n), F32), array((rows, n), F32), array((count * members, n), F32)]
        + [array(t.shape, BF16) for t in plan.x_table],
        [pltpu.SemaphoreType.DMA((3,))],
    )(offset, mixing, probes.reshape(1, -1), observed.reshape(1, -1), *map(in_hbm, plan.x_table), blocks[1])
    line = local(
        functools.partial(member_kernel, plan), "member_step", 24, [SMEM] + [HBM] * 3 + [VMEM] * (3 + space),
        array((space, plan.block, 2 * rows), F32),
        [pltpu.VMEM((space,) + block_shape, F32), pltpu.VMEM(plan.y_inverse.shape, BF16),
         pltpu.VMEM(plan.y_own.shape[1:], BF16), pltpu.VMEM(plan.x_inverse.shape, BF16),
         pltpu.VMEM((4, plan.modes, plan.kpad), F32), pltpu.SemaphoreType.DMA((3,))],
    )(me, *map(in_hbm, (plan.y_inverse, plan.y_own, plan.x_inverse)), *x_table, *blocks)
    moved = exchange(line)
    rounded = local(
        functools.partial(finish_kernel, plan), "modes_to_rows", 8, [VMEM] * 5, array((count, rows, n), BF16)
    )(moved, driving_source, *plan.y_table)
    values = lax.all_gather(rounded, "member", axis=0, tiled=True)
    analysis, part = local(
        analysis_kernel, "analysis", 16, [VMEM] * 4,
        [array((count, rows, n), F32), array((space, members, LANES), F32)],
        [pltpu.VMEM((members + 1, members, LANES), F32), pltpu.VMEM((count, rows, n), F32), pltpu.SemaphoreType.DMA(())],
        [HBM, VMEM],
    )(values, weights, number, total)
    parts = exchange(part)
    spread, projection = local(
        functools.partial(total_kernel, probes.shape[0] * space), "probe_totals", 4, [VMEM],
        [array((members, members), F32), array((1, members), F32)],
    )(parts)
    return analysis, spread, projection.reshape(members)


def solution(mesh):
    space = mesh.shape["space"]

    def body(participant_swirls, *rest):
        count, rows, n = participant_swirls.shape
        return on_device(Plan(n, rows, space, count), participant_swirls, *rest)

    return jax.shard_map(
        body,
        mesh=mesh,
        in_specs=(P("member", "space", None), P("space", None), P(), P("space"), P("space")),
        out_specs=(P("member", "space", None), P(), P()),
        check_vma=False,
    )
```
